256 devices in a mesh: rep: 16 (over z_hi, x), tp: 16 (over z_lo, y, core).
Axes of the slice: x: 4, y: 4, z: 8 (z_hi: 4, z_lo: 2; z = z_hi * 2 + z_lo), core: 2. Of those that a mesh axis runs over, the one named last changes fastest.
Arguments:
- tokens: bfloat16 [512, 4096], P(('rep', 'tp')), may hold values from -6 to 6
- conv_state: bfloat16 [3, 512, 8192], P(None, 'rep', 'tp'), may hold values from -6 to 6
- ssm_state: float32 [512, 16, 8192], P('rep', None, 'tp'), may hold values from -6 to 6
- norm_gains: bfloat16 [2, 4096], P(None, ('rep', 'tp')), may hold values from 0.5 to 1.5
- conv_weight: bfloat16 [4, 8192], P(None, ('rep', 'tp')), may hold values from -3 to 3
- conv_skip: bfloat16 [2, 8192], P(None, ('rep', 'tp')), may hold values from -3 to 3
- step_bias: bfloat16 [8192], P(('rep', 'tp')), may hold values from -5 to -1
- decay_log: bfloat16 [16, 8192], P(None, ('rep', 'tp')), may hold values from 0 to 2.796875
- input_proj: bfloat16 [4096, 2, 8192], P(('rep', 'tp')), may hold values from -0.09375 to 0.09375
- select_proj: bfloat16 [8192, 288], P('tp', 'rep'), may hold values from -0.0625 to 0.0625
- step_proj: bfloat16 [256, 8192], P(('rep', 'tp')), may hold values from -0.375 to 0.375
- output_proj: bfloat16 [8192, 4096], P(None, ('rep', 'tp')), may hold values from -0.0625 to 0.0625
- router: bfloat16 [4096, 16], P(('rep', 'tp')), may hold values from -0.09375 to 0.09375
- expert_proj: bfloat16 [4096, 2, 2, 12288], P(('rep', 'tp')), may hold values from -0.09375 to 0.09375
- expert_ids: int32 [512, 2], P(('rep', 'tp')), may hold values from 0 to 15, as said below
Outputs:
- mamba_out: bfloat16 [512, 4096], P(('rep', 'tp'))
- conv_next: bfloat16 [3, 512, 8192], P(None, 'rep', 'tp')
- ssm_next: float32 [512, 16, 8192], P('rep', None, 'tp')
- expert_hidden: bfloat16 [1024, 12288], P('rep', 'tp')
The draws below stay inside these ranges and needn't reach their ends.
Inputs may be any that keep to these rules, and one draw needn't show every extreme that they name: `expert_ids`: each row names two different experts. Within each aligned block of 2 rows (the rows of one device) each expert e < 2 is named by at most 2 rows.
All inputs are finite; a program needn't handle non-finite values.
Results may differ from the reference program's by a relative error of at most 0.04.
Values may be sent and summed in bfloat16 or wider, within the bound.
A program may use at most 128 MiB of HBM per device.

```python
import jax
import jax.numpy as jnp
from jax import lax

D = 4096
INNER = 8192
STEP_RANK = 256
STATE = 16
TAPS = 4
FF = 12288
EXPERTS = 16
EXP_WIN = 2
CAPACITY = 2
TOK_DEV = 2
REQ = 32
TOKENS = 512
SLOTS = 1024
N_REP = 16
N_TP = 16


def draw_expert_ids(key, part):
    blocks = TOKENS // TOK_DEV
    per_replica = REQ // TOK_DEV
    subkeys = jax.random.split(jax.random.fold_in(key, 17), 6)
    counts = jax.random.randint(subkeys[0], (blocks, EXP_WIN), 1, CAPACITY + 1)
    full_replica = jax.random.randint(subkeys[1], (), 0, blocks // per_replica)
    replica_of = jnp.arange(blocks, dtype=jnp.int32) // per_replica
    counts = jnp.where((replica_of == full_replica)[:, None], CAPACITY, counts)
    scores = jax.random.randint(subkeys[2], (blocks, TOK_DEV, EXP_WIN), 0, 1 << 20) * TOK_DEV + jnp.arange(TOK_DEV, dtype=jnp.int32)[None, :, None]
    ordering = jnp.argsort(scores, axis=1)
    order_rank = jnp.argsort(ordering, axis=1)
    member = order_rank < counts[:, None, :]
    in_first = member[:, :, 0]
    in_second = member[:, :, 1]
    spare = EXPERTS - EXP_WIN
    spare_one = EXP_WIN + jax.random.randint(subkeys[3], (blocks, TOK_DEV), 0, spare)
    spare_two = EXP_WIN + (spare_one - EXP_WIN + jax.random.randint(subkeys[4], (blocks, TOK_DEV), 1, spare)) % spare
    first_pick = jnp.where(in_first, 0, jnp.where(in_second, 1, spare_one))
    second_pick = jnp.where(in_first & in_second, 1, jnp.where(in_first | in_second, spare_one, spare_two))
    swapped = jax.random.randint(subkeys[5], (blocks, TOK_DEV), 0, 2) == 1
    column_one = jnp.where(swapped, second_pick, first_pick)
    column_two = jnp.where(swapped, first_pick, second_pick)
    return jnp.stack([column_one, column_two], axis=-1).reshape(TOKENS, 2).astype(jnp.int32)


def shard_levels(key, extent, cuts, least, top_value):
    def one(axis_at, blocks):
        draws = jax.random.uniform(jax.random.fold_in(jax.random.fold_in(key, 6), axis_at), (blocks,), jnp.float32, least / len(cuts), top_value / len(cuts))
        return jnp.repeat(jnp.exp(draws), extent[axis_at] // blocks).reshape((-1,) + (1,) * (len(extent) - axis_at - 1))

    level = one(*cuts[0])
    for cut in cuts[1:]:
        level = level * one(*cut)
    return level


def normal_values(own_key, dims, scale, bound, cuts=(), held_as=jnp.bfloat16):
    level = shard_levels(own_key, dims, cuts, -0.22, 0.18) if cuts else 1.0
    array = jax.random.normal(own_key, dims, jnp.float32) * scale * level
    return jnp.minimum(jnp.maximum(array, -bound), bound).astype(held_as)


def setup_inputs(seed: int = 0) -> dict:
    splits = jax.random.split(jax.random.key(seed), 16)
    return {
        "tokens": normal_values(splits[0], (TOKENS, D), 1.0, 6.0, ((0, 256),)),
        "conv_state": normal_values(splits[1], (TAPS - 1, TOKENS, INNER), 1.0, 6.0, ((1, 16), (2, 16))),
        "ssm_state": normal_values(splits[2], (TOKENS, STATE, INNER), 1.0, 6.0, ((0, 16), (2, 16)), jnp.float32),
        "norm_gains": jnp.clip(1.0 + 0.1 * jax.random.normal(splits[3], (2, D), jnp.float32), 0.5, 1.5).astype(jnp.bfloat16),
        "conv_weight": normal_values(splits[4], (TAPS, INNER), 0.5, 3.0, ((1, 256),)),
        "conv_skip": normal_values(splits[5], (2, INNER), 0.5, 3.0, ((1, 256),)),
        "step_bias": jnp.clip(-5.0 + 4.0 * jax.random.uniform(splits[6], (INNER,), jnp.float32) ** shard_levels(splits[6], (INNER,), ((0, 256),), -0.2, 0.2), -5.0, -1.0).astype(jnp.bfloat16),
        "decay_log": jnp.clip(2.796875 * jax.random.uniform(splits[7], (STATE, INNER), jnp.float32) ** shard_levels(splits[7], (STATE, INNER), ((1, 256),), -0.2, 0.2), 0.0, 2.796875).astype(jnp.bfloat16),
        "input_proj": normal_values(splits[8], (D, 2, INNER), D ** -0.5, 0.09375, ((0, 256),)),
        "select_proj": normal_values(splits[9], (INNER, STEP_RANK + 2 * STATE), INNER ** -0.5, 0.0625, ((0, 16), (1, 16))),
        "step_proj": normal_values(splits[10], (STEP_RANK, INNER), STEP_RANK ** -0.5, 0.375, ((0, 256),)),
        "output_proj": normal_values(splits[11], (INNER, D), INNER ** -0.5, 0.0625, ((1, 256),)),
        "router": normal_values(splits[12], (D, EXPERTS), D ** -0.5, 0.09375, ((0, 256),)),
        "expert_proj": normal_values(splits[13], (D, EXP_WIN, 2, FF), D ** -0.5, 0.09375, ((0, 256),)),
        "expert_ids": draw_expert_ids(jax.random.fold_in(splits[15], 71), 0),
    }


epsilon = 1e-05

def norm_scale(values, gain):
    mean_square = lax.optimization_barrier(jnp.mean(values * values, axis=-1, keepdims=True))
    return values * lax.rsqrt(mean_square + epsilon) * gain.astype(jnp.float32)

def ssm_block(block_args):
    state, step_size, activated, input_map, output_map, decay_rate = block_args
    factor = jnp.exp(step_size[:, None, :] * decay_rate[None])
    state_next = factor * state + (step_size * activated)[:, None, :] * input_map[:, :, None]
    readout = lax.optimization_barrier(jnp.sum(state_next * output_map[:, :, None], axis=1))
    return (state_next, readout)

def reference(tokens, conv_state, ssm_state, norm_gains, conv_weight, conv_skip, step_bias, decay_log, input_proj, select_proj, step_proj, output_proj, router, expert_proj, expert_ids):
    residual_in = tokens.astype(jnp.float32)
    normed = norm_scale(residual_in, norm_gains[0]).astype(jnp.bfloat16)
    projected = jnp.dot(normed, input_proj.reshape(D, 2 * INNER), preferred_element_type=jnp.float32)
    conv_input = projected[:, :INNER]
    gate_z = projected[:, INNER:]
    conv_taps = conv_weight.astype(jnp.float32)
    history = conv_state.astype(jnp.float32)
    conv_mix = lax.optimization_barrier(jnp.sum(conv_taps[:-1, None, :] * history, axis=0)) + conv_taps[-1] * conv_input + conv_skip[0].astype(jnp.float32)
    conv_next = jnp.concatenate([conv_state[1:], conv_input.astype(jnp.bfloat16)[None]], axis=0)
    activated = jax.nn.silu(conv_mix)
    selected = jnp.dot(activated.astype(jnp.bfloat16), select_proj, preferred_element_type=jnp.float32)
    step_low = selected[:, :STEP_RANK].astype(jnp.bfloat16)
    input_map = selected[:, STEP_RANK:STEP_RANK + STATE]
    output_map = selected[:, STEP_RANK + STATE:]
    step_size = jax.nn.softplus(jnp.dot(step_low, step_proj, preferred_element_type=jnp.float32) + step_bias.astype(jnp.float32))
    decay_rate = -jnp.exp(decay_log.astype(jnp.float32))
    replicas = TOKENS // REQ
    state_next, readout = lax.map(lambda block_args: ssm_block(block_args + (decay_rate,)), (ssm_state.reshape(replicas, REQ, STATE, INNER), step_size.reshape(replicas, REQ, INNER), activated.reshape(replicas, REQ, INNER), input_map.reshape(replicas, REQ, STATE), output_map.reshape(replicas, REQ, STATE)))
    ssm_next = state_next.reshape(TOKENS, STATE, INNER)
    readout = readout.reshape(TOKENS, INNER) + conv_skip[1].astype(jnp.float32) * activated
    gated_out = (readout * jax.nn.silu(gate_z)).astype(jnp.bfloat16)
    inner_block = INNER // N_TP
    mixer_out = jnp.zeros((TOKENS, D), jnp.float32)
    for block_index in range(N_TP):
        lower = block_index * inner_block
        partial_out = jnp.dot(gated_out[:, lower:lower + inner_block], output_proj[lower:lower + inner_block], preferred_element_type=jnp.float32)
        mixer_out = mixer_out + lax.optimization_barrier(partial_out.astype(jnp.bfloat16)).astype(jnp.float32)
    residual = residual_in + mixer_out
    mamba_out = residual.astype(jnp.bfloat16)
    moe_in = norm_scale(residual, norm_gains[1]).astype(jnp.bfloat16)
    logits = jnp.dot(moe_in, router, preferred_element_type=jnp.float32)
    choose = (expert_ids[:, :, None] == jnp.arange(EXPERTS, dtype=jnp.int32)[None, None, :]).astype(jnp.float32)
    picked = lax.optimization_barrier(jnp.sum(choose * logits[:, None, :], axis=2))
    first_gate = jax.nn.sigmoid(picked[:, 0] - picked[:, 1])
    second_gate = jax.nn.sigmoid(picked[:, 1] - picked[:, 0])
    window = jnp.arange(EXP_WIN, dtype=jnp.int32)
    names_first = expert_ids[:, 0:1] == window[None, :]
    names_second = expert_ids[:, 1:2] == window[None, :]
    zero = jnp.zeros((), jnp.float32)
    gate_w = jnp.where(names_first, first_gate[:, None], zero) + jnp.where(names_second, second_gate[:, None], zero)
    routed = (names_first | names_second).astype(jnp.int32)
    blocks = TOKENS // TOK_DEV
    routed_blocks = routed.reshape(blocks, TOK_DEV, EXP_WIN)
    position = jnp.cumsum(routed_blocks, axis=1) - routed_blocks
    slot_of = ((position[..., None] == jnp.arange(CAPACITY, dtype=jnp.int32)) & (routed_blocks[..., None] > 0)).astype(jnp.float32)
    slot_x = jnp.einsum('btec,btd->becd', slot_of, moe_in.reshape(blocks, TOK_DEV, D).astype(jnp.float32)).astype(jnp.bfloat16)
    slot_gate = jnp.einsum('btec,bte->bec', slot_of, gate_w.reshape(blocks, TOK_DEV, EXP_WIN)).astype(jnp.bfloat16)
    feature_block = D // N_REP
    hidden_list = []
    for expert in range(EXP_WIN):
        slot_rows = slot_x[:, expert].reshape(blocks * CAPACITY, D)
        gate_up = jnp.zeros((blocks * CAPACITY, 2 * FF), jnp.float32)
        for block_index in range(N_REP):
            lower = block_index * feature_block
            partial_up = jnp.dot(slot_rows[:, lower:lower + feature_block], expert_proj[lower:lower + feature_block, expert].reshape(feature_block, 2 * FF), preferred_element_type=jnp.float32)
            gate_up = gate_up + lax.optimization_barrier(partial_up.astype(jnp.bfloat16)).astype(jnp.float32)
        slot_scale = slot_gate[:, expert].reshape(blocks * CAPACITY).astype(jnp.float32)
        hidden = slot_scale[:, None] * jax.nn.silu(gate_up[:, :FF]) * gate_up[:, FF:]
        hidden_list.append(hidden.reshape(blocks, CAPACITY, FF))
    expert_hidden = jnp.stack(hidden_list, axis=1).reshape(SLOTS, FF).astype(jnp.bfloat16)
    return (mamba_out, conv_next, ssm_next, expert_hidden)
```

```python
import functools

import jax
import jax.numpy as jnp
from jax import lax
from jax.experimental import pallas as pl
from jax.experimental.pallas import tpu as pltpu
from jax.sharding import Mesh
from jax.sharding import PartitionSpec as P

CAPACITY = 2
REP = ("rep_0", "rep_1")
REP_TP = ("rep_0", "rep_1", "tp")
MESH = pl.DeviceIdType.MESH
EPS = 1e-05
bf16 = jnp.bfloat16
f32 = jnp.float32
LANES = 128

PHASES = (
    "x1", "rs", "wi", "rg", "x2", "wo", "st", "prz", "sez", "prx",
    "sex", "pr2", "stz", "stx", "p3x", "p3z", "we", "sel", "gz", "gx",
    "mo", "mc", "y1", "info", "y2", "lx", "lz", "ex0", "ex1", "ex2",
    "ex3", "ez0", "ez1", "ez2", "ez3",
)
PH = {name: k for k, name in enumerate(PHASES)}


def sigmoid(v):
    return 1.0 / (1.0 + jnp.exp(-v))


def silu(v):
    return v / (1.0 + jnp.exp(-v))


def softplus(v):
    return jnp.maximum(v, 0.0) + jnp.log1p(jnp.exp(-jnp.abs(v)))


def dot(a, b):
    return jnp.dot(a, b, preferred_element_type=f32)


def dot_nt(a, b):
    return lax.dot_general(a, b, (((1,), (1,)), ((), ())), preferred_element_type=f32)


def kernel(
    nz, nx, nt,
    tokens, conv_state, ssm_state, input_proj, expert_proj, output_t, step_row, select_t, packed,
    router_gain, info,
    mamba_out, conv_next, ssm_next, expert_hidden,
    x_s, x1, x2, xx, rs_s, rs_r, wi_s, wi_r, rg_r, wo_r, st_s, st_r, st_b, st_z, st_x, pr_z, pr_x, pr2,
    se_z, se_x, p3, p3x, p3zs, p3z, we_s, we_r, sel_s, sel_r, maps, step_b, act_b, ro_b, ga_s, g_z, g_x,
    mo_s, mo_r, mc_r, y_s, y1, y2, yy, info_s, info_r, lg, lgx, lgzs, lgz, pe, pex, pezs, pez,
    ssem, rsem,
):
    nr = nz * nx
    z, x, t = lax.axis_index("rep_0"), lax.axis_index("rep_1"), lax.axis_index("tp")
    r = z * nx + x
    rows = input_proj.shape[0]
    fb = rows * nt
    ch = ssm_state.shape[2]
    st = ssm_state.shape[1]
    td = tokens.shape[0]
    rq = td * nt
    rank = nr * nt
    hid = expert_proj.shape[3] // nt
    groups = {
        "tp": (nt, t, lambda p: {"tp": p}),
        "rep": (nr, r, lambda p: {"rep_0": p // nx, "rep_1": p % nx}),
        "x": (nx, x, lambda p: {"rep_1": p}),
        "z": (nz, z, lambda p: {"rep_0": p}),
    }
    sent = []

    def send(group, name, src, dst):
        n, me, dev = groups[group]
        k = PH[name]

        def body(step, carry):
            peer = (me + step) % n
            pltpu.make_async_remote_copy(
                src_ref=src(peer), dst_ref=dst.at[me], send_sem=ssem.at[k], recv_sem=rsem.at[k],
                device_id=dev(peer), device_id_type=MESH,
            ).start()
            return carry

        lax.fori_loop(1, n, body, 0)
        pltpu.make_async_copy(src(me), dst.at[me], rsem.at[k]).start()
        sent.append((k, dst, n))

    def arrived(name, dst):
        pltpu.make_async_copy(dst, dst, rsem.at[PH[name]]).wait()

    def cols(ref, p, width):
        return ref.at[:, pl.ds(pl.multiple_of(p * width, width), width)]

    xv = tokens[...]
    for q in range(nr):
        x_s[q] = xv[:, q * fb : (q + 1) * fb]
    send("rep", "x1", lambda p: x_s.at[p], x1)
    xf = xv.astype(f32)
    rs = lax.rsqrt(jnp.mean(xf * xf, axis=1, keepdims=True) + EPS)
    rs_s[...] = jnp.broadcast_to(rs, (td, LANES))
    send("tp", "rs", lambda p: rs_s, rs_r)
    for j in range(2):
        wi_s[j * rows : (j + 1) * rows, :] = input_proj[:, j, :]
    send("tp", "wi", lambda p: cols(wi_s, p, ch), wi_r)
    send("tp", "rg", lambda p: router_gain, rg_r)
    send("z", "prz", lambda p: packed, pr_z)
    send("z", "sez", lambda p: select_t, se_z)
    arrived("x1", x1)
    send("tp", "x2", lambda p: x1, x2)
    at_row = lax.broadcasted_iota(jnp.int32, (nt, 1), 0) == t
    st_s[...] = jnp.where(at_row, step_row[...].astype(f32), 0.0).astype(bf16)
    send("tp", "st", lambda p: cols(st_s, p, ch), st_r)
    send("tp", "wo", lambda p: cols(output_t, p, ch), wo_r)
    arrived("prz", pr_z)
    send("x", "prx", lambda p: pr_z, pr_x)
    arrived("sez", se_z)
    send("x", "sex", lambda p: se_z, se_x)
    for e in range(2):
        for j in range(2):
            q = 2 * e + j
            we_s[q * rows : (q + 1) * rows, :] = expert_proj[:, e, j, :]

    arrived("rg", rg_r)
    rgv = rg_r[...].reshape(fb, LANES)
    rgt = rgv.astype(f32).T
    gain0 = rgt[16:17, :]
    gain1 = rgt[17:18, :]
    arrived("x2", x2)

    def place(src, gain, dst):
        def body(q, carry):
            block = src[:, q].reshape(rq, fb).astype(f32)
            dst[q % nx, q // nx] = (block * gain).astype(bf16)
            return carry

        lax.fori_loop(0, nr, body, 0)

    place(x2, gain0, xx)
    arrived("wi", wi_r)
    lhs = xx[...].reshape(nr * rq, fb)
    for j in range(2):
        w = wi_r[:, j * rows : (j + 1) * rows, :].reshape(fb, ch)
        p3[:, :, :, j * ch : (j + 1) * ch] = dot(lhs, w).astype(bf16).reshape(nx, nz, rq, ch)
    send("x", "p3x", lambda p: p3.at[p], p3x)
    send("tp", "we", lambda p: cols(we_s, p, hid), we_r)

    arrived("st", st_r)
    st_b[...] = jnp.sum(st_r[...].astype(f32), axis=0).astype(bf16)
    send("z", "stz", lambda p: st_b, st_z)
    arrived("prx", pr_x)
    send("tp", "pr2", lambda p: pr_x.at[p % nx, p // nx], pr2)
    arrived("stz", st_z)
    send("x", "stx", lambda p: st_z, st_x)
    arrived("sex", se_x)
    srw = select_t.shape[0]
    sp = sel_s.shape[1]
    width = (rank + 2 * st) // nr
    shape = (sp, nr * srw)
    at_col = lax.broadcasted_iota(jnp.int32, shape, 0)
    place_of = lax.broadcasted_iota(jnp.int32, shape, 1)
    blk, off = place_of // srw, place_of % srw
    true_col = ((blk % nz) * nx + blk // nz) * width + off
    perm = jnp.where((true_col == at_col) & (off < width), 1.0, 0.0).astype(bf16)
    select_all = dot(perm, se_x[...].reshape(nr * srw, ch)).astype(bf16)
    arrived("rs", rs_r)
    rsv = rs_r[...].reshape(rq, LANES)[:, 0:1]

    arrived("p3x", p3x)
    acc = p3x[0].astype(f32)
    for k in range(1, nx):
        acc = acc + p3x[k].astype(f32)
    p3zs[...] = acc.astype(bf16)
    send("z", "p3z", lambda p: p3zs.at[p], p3z)
    arrived("pr2", pr2)
    par = pr2[...].reshape(ch, LANES).astype(f32).T
    history = jnp.sum(par[0:3][:, None, :] * conv_state[...].astype(f32), axis=0) + par[4:5]
    decay_rate = -jnp.exp(par[7 : 7 + st])
    conv_next[0] = conv_state[1]
    conv_next[1] = conv_state[2]
    arrived("p3z", p3z)
    acc = p3z[0].astype(f32)
    for k in range(1, nz):
        acc = acc + p3z[k].astype(f32)
    projected = acc * rsv
    conv_input = projected[:, :ch]
    gate_z = projected[:, ch:]
    conv_next[2] = conv_input.astype(bf16)
    activated = silu(history + par[3:4] * conv_input)
    sel_s[...] = dot_nt(activated.astype(bf16), select_all).astype(bf16)
    send("tp", "sel", lambda p: sel_s, sel_r)
    arrived("stx", st_x)
    step_all = jnp.concatenate([st_x[q % nx, q // nx] for q in range(nr)], axis=0)
    act_b[...] = activated
    arrived("sel", sel_r)
    selected = jnp.sum(sel_r[...].astype(f32), axis=0)
    step_low = selected[:, :rank].astype(bf16)
    maps[...] = jnp.broadcast_to(selected[:, rank : rank + 2 * st][:, :, None], maps.shape)
    step_b[...] = softplus(dot(step_low, step_all) + par[6:7])

    def token(i, carry):
        s = step_b[pl.ds(i, 1), :]
        a = act_b[pl.ds(i, 1), :]
        m = maps[i]
        wide = jnp.concatenate([m] * (ch // LANES), axis=1)
        nxt = jnp.exp(s * decay_rate) * ssm_state[i] + (s * a) * wide[:st]
        ssm_next[i] = nxt
        ro_b[pl.ds(i, 1), :] = jnp.sum(nxt * wide[st:], axis=0, keepdims=True)
        return carry

    lax.fori_loop(0, rq, token, 0)
    readout = ro_b[...] + par[5:6] * activated
    ga_s[...] = (readout * silu(gate_z)).astype(bf16)

    send("z", "gz", lambda p: ga_s, g_z)
    arrived("gz", g_z)
    send("x", "gx", lambda p: g_z, g_x)
    arrived("wo", wo_r)
    arrived("gx", g_x)
    mo = dot_nt(g_x[...].reshape(nr * rq, ch), wo_r[...].reshape(fb, ch))
    mo_s[...] = mo.astype(bf16).reshape(nx, nz, nt, td, fb)
    send("rep", "mo", lambda p: mo_s.at[p % nx, p // nx], mo_r)
    arrived("mo", mo_r)
    send("tp", "mc", lambda p: mo_r.at[:, p], mc_r)
    arrived("mc", mc_r)
    acc = x_s[...].astype(f32)
    for k in range(nt):
        acc = acc + mc_r[k].astype(f32)
    y_s[...] = acc.astype(bf16)
    send("rep", "y1", lambda p: y_s.at[p], y1)
    square = jnp.sum(jnp.sum(acc * acc, axis=0), axis=1, keepdims=True)
    rs2 = lax.rsqrt(square * (1.0 / (nr * fb)) + EPS)
    lane = lax.broadcasted_iota(jnp.int32, (td, LANES), 1)
    info_s[...] = jnp.where(lane == 0, rs2, info[...])
    send("tp", "info", lambda p: info_s, info_r)
    for q in range(nr):
        mamba_out[:, q * fb : (q + 1) * fb] = y_s[q]

    arrived("y1", y1)
    send("tp", "y2", lambda p: y1, y2)
    arrived("we", we_r)
    arrived("y2", y2)
    place(y2, gain1, yy)
    lhs2 = yy[...].reshape(nr * rq, fb)
    lg[...] = dot(lhs2, rgv).astype(bf16).reshape(nx, nz, rq, LANES)
    send("x", "lx", lambda p: lg.at[p], lgx)
    for q in range(4):
        w = we_r[:, q * rows : (q + 1) * rows, :].reshape(fb, hid)
        pe[q] = dot(lhs2, w).astype(bf16).reshape(nx, nz, rq, hid)
        send("x", "ex%d" % q, lambda p, q=q: pe.at[q, p], pex.at[q])

    arrived("lx", lgx)
    acc = lgx[0].astype(f32)
    for k in range(1, nx):
        acc = acc + lgx[k].astype(f32)
    lgzs[...] = acc.astype(bf16)
    send("z", "lz", lambda p: lgzs.at[p], lgz)
    for q in range(4):
        arrived("ex%d" % q, pex.at[q])
        acc = pex[q, 0].astype(f32)
        for k in range(1, nx):
            acc = acc + pex[q, k].astype(f32)
        pezs[q] = acc.astype(bf16)
        send("z", "ez%d" % q, lambda p, q=q: pezs.at[q, p], pez.at[q])

    arrived("info", info_r)
    arrived("lz", lgz)
    acc = lgz[0].astype(f32)
    for k in range(1, nz):
        acc = acc + lgz[k].astype(f32)
    inf = info_r[...].reshape(rq, LANES)
    scale = inf[:, 0:1]
    id0, id1 = inf[:, 1:2], inf[:, 2:3]
    logits = acc * scale
    lane = lax.broadcasted_iota(jnp.int32, (rq, LANES), 1).astype(f32)
    zero = jnp.zeros((), f32)
    first = jnp.sum(jnp.where(lane == id0, logits, zero), axis=1, keepdims=True)
    second = jnp.sum(jnp.where(lane == id1, logits, zero), axis=1, keepdims=True)
    gate_first = sigmoid(first - second)
    gate_second = sigmoid(second - first)
    inft = inf.T
    slots = 2 * CAPACITY * nt
    slot = lax.broadcasted_iota(jnp.int32, (slots, rq), 0).astype(f32)
    token_at = lax.broadcasted_iota(jnp.int32, (slots, rq), 1)
    base = ((token_at // td) * (2 * CAPACITY)).astype(f32)
    total = jnp.zeros((slots, hid), f32)
    for e in range(2):
        gate = jnp.where(id0 == e, gate_first, zero) + jnp.where(id1 == e, gate_second, zero)
        gate = gate.astype(bf16).astype(f32)
        halves = []
        for j in range(2):
            q = 2 * e + j
            arrived("ez%d" % q, pez.at[q])
            acc = pez[q, 0].astype(f32)
            for k in range(1, nz):
                acc = acc + pez[q, k].astype(f32)
            halves.append(acc * scale)
        hidden = (gate * silu(halves[0]) * halves[1]).astype(bf16)
        want = inft[3 + e : 4 + e, :]
        pick = jnp.where((slot == base + want) & (want >= 0.0), 1.0, 0.0).astype(bf16)
        total = total + dot(pick, hidden)
    expert_hidden[...] = total.astype(bf16)

    for k, dst, n in sent:
        part = dst.at[pl.ds(0, n - 1)]
        pltpu.make_async_copy(part, part, ssem.at[k]).wait()


def shards(
    nz, nx, nt, tokens, conv_state, ssm_state, norm_gains, conv_weight, conv_skip, step_bias, decay_log,
    input_proj, select_proj, step_proj, output_proj, router, expert_proj, expert_ids,
):
    nr = nz * nx
    rows = input_proj.shape[0]
    td, model = tokens.shape
    rq = td * nt
    fb = rows * nt
    _, st, ch = ssm_state.shape
    hid = expert_proj.shape[3] // nt
    cdev = conv_weight.shape[1]

    packed = jnp.concatenate([conv_weight, conv_skip, step_bias[None], decay_log], axis=0).T
    packed = jnp.pad(packed, ((0, 0), (0, LANES - packed.shape[1])))
    router_gain = jnp.concatenate([router, norm_gains.T], axis=1)
    router_gain = jnp.pad(router_gain, ((0, 0), (0, LANES - router_gain.shape[1])))
    select_t = select_proj.T
    srw = -(-select_t.shape[0] // 16) * 16
    sp = -(-select_t.shape[0] * nr // LANES) * LANES
    select_t = jnp.pad(select_t, ((0, srw - select_t.shape[0]), (0, 0)))
    window = jnp.arange(2, dtype=jnp.int32)
    routed = ((expert_ids[:, 0:1] == window) | (expert_ids[:, 1:2] == window)).astype(jnp.int32)
    position = jnp.cumsum(routed, axis=0) - routed
    want = jnp.where(routed > 0, window * CAPACITY + position, -1)
    info = jnp.concatenate([jnp.zeros((td, 1), jnp.int32), expert_ids, want], axis=1).astype(f32)
    info = jnp.pad(info, ((0, 0), (0, LANES - info.shape[1])))

    V = pltpu.VMEM
    scratch = dict(
        x_s=((nr, td, fb), bf16), x1=((nr, td, fb), bf16), x2=((nt, nr, td, fb), bf16),
        xx=((nx, nz, rq, fb), bf16),
        rs_s=((td, LANES), f32), rs_r=((nt, td, LANES), f32),
        wi_s=((2 * rows, nt * ch), bf16), wi_r=((nt, 2 * rows, ch), bf16),
        rg_r=((nt, rows, LANES), bf16),
        wo_r=((nt, output_proj.shape[1], ch), bf16),
        st_s=((nt, nt * ch), bf16), st_r=((nt, nt, ch), bf16), st_b=((nt, ch), bf16),
        st_z=((nz, nt, ch), bf16), st_x=((nx, nz, nt, ch), bf16),
        pr_z=((nz, cdev, LANES), bf16), pr_x=((nx, nz, cdev, LANES), bf16), pr2=((nt, cdev, LANES), bf16),
        se_z=((nz, srw, ch), bf16), se_x=((nx, nz, srw, ch), bf16),
        p3=((nx, nz, rq, 2 * ch), bf16), p3x=((nx, nz, rq, 2 * ch), bf16),
        p3zs=((nz, rq, 2 * ch), bf16), p3z=((nz, rq, 2 * ch), bf16),
        we_s=((4 * rows, nt * hid), bf16), we_r=((nt, 4 * rows, hid), bf16),
        sel_s=((rq, sp), bf16), sel_r=((nt, rq, sp), bf16),
        maps=((rq, 2 * st, LANES), f32), step_b=((rq, ch), f32), act_b=((rq, ch), f32),
        ro_b=((rq, ch), f32),
        ga_s=((rq, ch), bf16), g_z=((nz, rq, ch), bf16), g_x=((nx, nz, rq, ch), bf16),
        mo_s=((nx, nz, nt, td, fb), bf16), mo_r=((nr, nt, td, fb), bf16),
        mc_r=((nt, nr, td, fb), bf16), y_s=((nr, td, fb), bf16), y1=((nr, td, fb), bf16),
        y2=((nt, nr, td, fb), bf16), yy=((nx, nz, rq, fb), bf16),
        info_s=((td, LANES), f32), info_r=((nt, td, LANES), f32),
        lg=((nx, nz, rq, LANES), bf16), lgx=((nx, nz, rq, LANES), bf16),
        lgzs=((nz, rq, LANES), bf16), lgz=((nz, rq, LANES), bf16),
        pe=((4, nx, nz, rq, hid), bf16), pex=((4, nx, nz, rq, hid), bf16),
        pezs=((4, nz, rq, hid), bf16), pez=((4, nz, rq, hid), bf16),
    )
    scratch_shapes = [V(s, d) for s, d in scratch.values()]
    scratch_shapes += [pltpu.SemaphoreType.DMA((len(PHASES),))] * 2
    operands = (
        tokens, conv_state, ssm_state, input_proj, expert_proj, output_proj.T, step_proj, select_t, packed,
        router_gain, info,
    )
    return pl.pallas_call(
        functools.partial(kernel, nz, nx, nt),
        out_shape=(
            jax.ShapeDtypeStruct((td, model), bf16),
            jax.ShapeDtypeStruct(conv_state.shape, bf16),
            jax.ShapeDtypeStruct(ssm_state.shape, f32),
            jax.ShapeDtypeStruct((2 * CAPACITY * nt, hid), bf16),
        ),
        in_specs=[pl.BlockSpec(memory_space=V)] * len(operands),
        out_specs=[pl.BlockSpec(memory_space=V)] * 4,
        scratch_shapes=scratch_shapes,
        compiler_params=pltpu.CompilerParams(has_side_effects=True, vmem_limit_bytes=60 * 1024 * 1024),
        name="step",
    )(*operands)


def solution(mesh, nz=4):
    devices = mesh.devices
    nx, nt = devices.shape[0] // nz, devices.shape[1]
    split = Mesh(devices.reshape(nz, nx, nt), REP_TP)
    return jax.shard_map(
        functools.partial(shards, nz, nx, nt),
        mesh=split,
        in_specs=(
            P(REP_TP, None),
            P(None, REP, "tp"),
            P(REP, None, "tp"),
            P(None, REP_TP),
            P(None, REP_TP),
            P(None, REP_TP),
            P(REP_TP),
            P(None, REP_TP),
            P(REP_TP, None, None),
            P("tp", REP),
            P(REP_TP, None),
            P(None, REP_TP),
            P(REP_TP, None),
            P(REP_TP, None, None, None),
            P(REP_TP, None),
        ),
        out_specs=(P(REP_TP, None), P(None, REP, "tp"), P(REP, None, "tp"), P(REP, "tp")),
        check_vma=False,
    )
```

```python
import functools

import jax
import jax.numpy as jnp
from jax import lax
from jax.experimental import pallas as pl
from jax.experimental.pallas import tpu as pltpu
from jax.sharding import Mesh
from jax.sharding import PartitionSpec as P

CAPACITY = 2
REP = ("rep_0", "rep_1")
REP_TP = ("rep_0", "rep_1", "tp")
MESH = pl.DeviceIdType.MESH
EPS = 1e-05
bf16 = jnp.bfloat16
f32 = jnp.float32
LANES = 128

PHASES = (
    "x1", "xb", "rs", "wi", "gn", "rg", "prz", "sez", "x2", "st",
    "wo", "we0", "we1", "stz", "p3x", "p3z", "prx", "sex", "pr2", "stx",
    "gnx", "rgx", "wox", "wex", "sel", "gz", "mc", "y2", "yo", "info",
    "lz", "yx1", "yx2", "yx3", "ez0", "ez1", "ez2", "ez3", "fin",
)
PH = {name: k for k, name in enumerate(PHASES)}


def sigmoid(v):
    return 1.0 / (1.0 + jnp.exp(-v))


def silu(v):
    return v / (1.0 + jnp.exp(-v))


def softplus(v):
    return jnp.maximum(v, 0.0) + jnp.log1p(jnp.exp(-jnp.abs(v)))


def dot(a, b):
    return jnp.dot(a, b, preferred_element_type=f32)


def dot_nt(a, b):
    return lax.dot_general(a, b, (((1,), (1,)), ((), ())), preferred_element_type=f32)


def kernel(
    nz, nx, nt,
    tokens, conv_state, ssm_state, norm_gains, conv_weight, conv_skip, step_bias, decay_log,
    input_proj, select_t, step_row, output_t, router, expert_proj, expert_ids,
    mamba_out, conv_next, ssm_next, expert_hidden,
    x1, xb, x2, xx, rs_s, rs_r, wi_s, wi_r, gn_s, gn_r, gn_b, gn_x, rg_s, rg_r, rg_x, wo_r, wo_x,
    st_s, st_r, st_b, st_z, st_x, pk, pr_s, pr_z, pr_x, pr2, se_s, se_z, se_x, p3, p3x, p3zs, p3z,
    we_s, we_r, we_x, sel_s, sel_r, maps, step_b, act_b, ro_b, ga_s, g_z,
    mo_s, mc_r, y_s, y2, yo, yx, info_s, info_r, lg, lgz, pe, pez, fin_s, fin,
    ssem, rsem,
):
    nr = nz * nx
    z, x, t = lax.axis_index("rep_0"), lax.axis_index("rep_1"), lax.axis_index("tp")
    r = z * nx + x
    rows = input_proj.shape[0]
    fb = rows * nt
    fz = fb * nx
    ch = ssm_state.shape[2]
    st = ssm_state.shape[1]
    td = tokens.shape[0]
    rq = td * nt
    rank = nr * nt
    hid = expert_proj.shape[3] // nt
    cdev = conv_weight.shape[1]
    per_x = 4 // nx
    groups = {
        "tp": (nt, t, lambda p: {"tp": p}),
        "rep": (nr, r, lambda p: {"rep_0": p // nx, "rep_1": p % nx}),
        "x": (nx, x, lambda p: {"rep_1": p}),
        "z": (nz, z, lambda p: {"rep_0": p}),
    }
    pending = []

    def remote(src, dst, k, device):
        pltpu.make_async_remote_copy(
            src_ref=src, dst_ref=dst, send_sem=ssem.at[k], recv_sem=rsem.at[k],
            device_id=device, device_id_type=MESH,
        ).start()

    def send(group, name, src, dst, at=None, part=None):
        n, me, dev = groups[group]
        k = PH[name]
        at = at or (lambda me: dst.at[me])

        def body(step, carry):
            peer = (me + step) % n
            remote(src(peer), at(me), k, dev(peer))
            return carry

        if n > 1:
            lax.fori_loop(1, n, body, 0)
            pending.append((k, dst.at[pl.ds(0, n - 1)] if part is None else part))
        pltpu.make_async_copy(src(me), at(me), rsem.at[k]).start()

    def arrived(name, dst):
        pltpu.make_async_copy(dst, dst, rsem.at[PH[name]]).wait()

    def cols(ref, p, width):
        return ref.at[:, pl.ds(pl.multiple_of(p * width, width), width)]

    def total(ref):
        acc = ref[0].astype(f32)
        for k in range(1, ref.shape[0]):
            acc = acc + ref[k].astype(f32)
        return acc

    barrier = pltpu.get_barrier_semaphore()
    for group in ("tp", "rep"):
        n, me, dev = groups[group]

        def greet(step, carry, n=n, me=me, dev=dev):
            pl.semaphore_signal(barrier, inc=1, device_id=dev((me + step) % n), device_id_type=MESH)
            return carry

        lax.fori_loop(1, n, greet, 0)

    for j in range(2):
        wi_s[j * rows : (j + 1) * rows, :] = input_proj[:, j, :]
    xf = tokens[...].astype(f32)
    rs = lax.rsqrt(jnp.mean(xf * xf, axis=1, keepdims=True) + EPS)
    rs_s[...] = jnp.broadcast_to(rs, (td, LANES))
    pl.semaphore_wait(barrier, nt - 1 + nr - 1)

    send("rep", "x1", lambda p: cols(tokens, p, fb), x1)
    send("tp", "wi", lambda p: cols(wi_s, p, ch), wi_r)
    gn_s[...] = jnp.zeros(gn_s.shape, bf16)
    gn_s[:, 0:rows] = norm_gains[...]
    send("tp", "gn", lambda p: gn_s, gn_r)
    send("tp", "rs", lambda p: rs_s, rs_r)
    at_row = lax.broadcasted_iota(jnp.int32, (nt, 1), 0) == t
    st_s[...] = jnp.where(at_row, step_row[...].astype(f32), 0.0).astype(bf16)
    pk[...] = jnp.zeros(pk.shape, f32)
    pk[0:4, 0:cdev] = conv_weight[...].astype(f32)
    pk[4:6, 0:cdev] = conv_skip[...].astype(f32)
    pk[6:7, 0:cdev] = step_bias[...].astype(f32)
    pk[7 : 7 + st, 0:cdev] = decay_log[...].astype(f32)
    pr_s[...] = pk[...].astype(bf16)
    se_s[...] = jnp.zeros(se_s.shape, bf16)
    se_s[0 : select_t.shape[0], :] = select_t[...]
    rg_s[...] = jnp.zeros(rg_s.shape, bf16)
    rg_s[:, 0 : router.shape[1]] = router[...]
    arrived("x1", x1)
    send("tp", "x2", lambda p: x1, x2)
    send("tp", "st", lambda p: cols(st_s, p, ch), st_r)
    send("z", "prz", lambda p: pr_s, pr_z)
    send("z", "sez", lambda p: se_s, se_z)
    send("z", "xb", lambda p: cols(tokens, p, fz), xb)
    send("tp", "rg", lambda p: rg_s, rg_r)
    send("tp", "wo", lambda p: cols(output_t, p, ch), wo_r)

    def send_experts(e):
        for j in range(2):
            we_s[2 * e + j] = expert_proj[:, e, j, :]
        half = we_r.at[pl.ds(2 * e, 2)]
        send(
            "tp", "we%d" % e,
            lambda p: we_s.at[pl.ds(2 * e, 2), :, pl.ds(pl.multiple_of(p * hid, hid), hid)], half,
            at=lambda me: half.at[:, me], part=half.at[:, pl.ds(0, nt - 1)],
        )

    send_experts(0)

    arrived("gn", gn_r)
    gnv = gn_r[...].astype(f32)
    gains = jnp.concatenate([gnv[k][:, 0:rows] for k in range(nt)], axis=1)
    gn_b[...] = gains.astype(bf16)
    gain0 = gains[0:1, :]
    arrived("x2", x2)

    def place_in(q, carry):
        block = x2[:, q].reshape(rq, fb).astype(f32)
        xx[q % nx, q // nx] = (block * gain0).astype(bf16)
        return carry

    lax.fori_loop(0, nr, place_in, 0)
    arrived("wi", wi_r)
    lhs = xx[...].reshape(nr * rq, fb)
    for j in range(2):
        w = wi_r[:, j * rows : (j + 1) * rows, :].reshape(fb, ch)
        p3[:, :, :, j * ch : (j + 1) * ch] = dot(lhs, w).astype(bf16).reshape(nx, nz, rq, ch)
    send("x", "p3x", lambda p: p3.at[p], p3x)

    arrived("st", st_r)
    st_b[...] = jnp.sum(st_r[...].astype(f32), axis=0).astype(bf16)
    send("z", "stz", lambda p: st_b, st_z)
    arrived("prz", pr_z)
    send("x", "prx", lambda p: pr_z, pr_x)
    arrived("sez", se_z)
    send("x", "sex", lambda p: se_z, se_x)
    send("x", "gnx", lambda p: gn_b, gn_x)
    arrived("rg", rg_r)
    send("x", "rgx", lambda p: rg_r, rg_x)
    arrived("wo", wo_r)
    send("x", "wox", lambda p: wo_r, wo_x)

    arrived("p3x", p3x)
    p3zs[...] = total(p3x).astype(bf16)
    send("z", "p3z", lambda p: p3zs.at[p], p3z)
    arrived("prx", pr_x)
    send("tp", "pr2", lambda p: pr_x.at[p % nx, p // nx], pr2)
    arrived("stz", st_z)
    send("x", "stx", lambda p: st_z, st_x)
    send_experts(1)
    arrived("sex", se_x)
    srw = se_s.shape[0]
    sp = sel_s.shape[1]
    width = select_t.shape[0]
    shape = (sp, nr * srw)
    at_col = lax.broadcasted_iota(jnp.int32, shape, 0)
    place_of = lax.broadcasted_iota(jnp.int32, shape, 1)
    blk, off = place_of // srw, place_of % srw
    true_col = ((blk % nz) * nx + blk // nz) * width + off
    perm = jnp.where((true_col == at_col) & (off < width), 1.0, 0.0).astype(bf16)
    select_all = dot(perm, se_x[...].reshape(nr * srw, ch)).astype(bf16)
    arrived("rs", rs_r)
    rsv = rs_r[...].reshape(rq, LANES)[:, 0:1]
    arrived("pr2", pr2)
    prv = pr2[...].astype(f32)
    par = jnp.concatenate([prv[k][:, 0:cdev] for k in range(nt)], axis=1)
    history = jnp.sum(par[0:3][:, None, :] * conv_state[...].astype(f32), axis=0) + par[4:5]
    decay_rate = -jnp.exp(par[7 : 7 + st])
    conv_next[0] = conv_state[1]
    conv_next[1] = conv_state[2]
    arrived("p3z", p3z)
    projected = total(p3z) * rsv
    conv_input = projected[:, :ch]
    gate_z = projected[:, ch:]
    conv_next[2] = conv_input.astype(bf16)
    activated = silu(history + par[3:4] * conv_input)
    sel_s[...] = dot_nt(activated.astype(bf16), select_all).astype(bf16)
    send("tp", "sel", lambda p: sel_s, sel_r)
    act_b[...] = activated
    for e in range(2):
        arrived("we%d" % e, we_r.at[pl.ds(2 * e, 2)])
    send("x", "wex", lambda p: we_r.at[pl.ds(p * per_x, per_x)], we_x)
    arrived("stx", st_x)
    step_all = jnp.concatenate([st_x[q % nx, q // nx] for q in range(nr)], axis=0)
    arrived("sel", sel_r)
    selected = total(sel_r)
    step_low = selected[:, :rank].astype(bf16)
    maps[...] = jnp.broadcast_to(selected[:, rank : rank + 2 * st][:, :, None], maps.shape)
    step_b[...] = softplus(dot(step_low, step_all) + par[6:7])

    def token(i, carry):
        s = step_b[pl.ds(i, 1), :]
        a = act_b[pl.ds(i, 1), :]
        m = maps[i]
        wide = jnp.concatenate([m] * (ch // LANES), axis=1)
        nxt = jnp.exp(s * decay_rate) * ssm_state[i] + (s * a) * wide[:st]
        ssm_next[i] = nxt
        ro_b[pl.ds(i, 1), :] = jnp.sum(nxt * wide[st:], axis=0, keepdims=True)
        return carry

    lax.fori_loop(0, rq, token, 0)
    readout = ro_b[...] + par[5:6] * activated
    ga_s[...] = (readout * silu(gate_z)).astype(bf16)

    send("z", "gz", lambda p: ga_s, g_z)
    arrived("wox", wo_x)
    arrived("gz", g_z)
    mo = dot_nt(g_z[...].reshape(nz * rq, ch), wo_x[...].reshape(fz, ch))
    mo_s[...] = mo.astype(bf16).reshape(nz, nt, td, fz)
    send("tp", "mc", lambda p: mo_s.at[:, p], mc_r)
    arrived("xb", xb)
    arrived("mc", mc_r)
    y_s[...] = (xb[...].astype(f32) + total(mc_r)).astype(bf16)
    send("tp", "y2", lambda p: y_s, y2)
    send("z", "yo", lambda p: y_s.at[p], yo)

    arrived("gnx", gn_x)
    gain1 = jnp.concatenate([gn_x[k].astype(f32)[1:2, :] for k in range(nx)], axis=1)
    arrived("rgx", rg_x)
    arrived("y2", y2)
    for q in range(nz):
        block = y2[:, q].reshape(rq, fz).astype(f32)
        yx[0, q] = (block * gain1).astype(bf16)
    for k in range(1, nx):
        remote(yx.at[0], yx.at[k], PH["yx%d" % k], {"rep_1": (x + k) % nx})
        pending.append((PH["yx%d" % k], yx.at[0]))
    arrived("wex", we_x)
    for k in range(nx):
        if k:
            arrived("yx%d" % k, yx.at[k])
        left = yx[k].reshape(nz * rq, fz)
        for c in range(per_x):
            part = dot(left, we_x[:, c].reshape(fz, hid))
            pe[k, :, c] = part.astype(bf16).reshape(nz, rq, hid)
        send("z", "ez%d" % k, lambda p, k=k: pe.at[k, p], pez.at[k])
        if k == 0:
            lg[...] = dot(left, rg_x[...].reshape(fz, LANES)).astype(bf16).reshape(nz, rq, LANES)
            send("z", "lz", lambda p: lg.at[p], lgz)

    arrived("yo", yo)
    yov = [yo[k].astype(f32) for k in range(nz)]
    square = jnp.zeros((td, 1), f32)
    for k in range(nz):
        mamba_out[:, k * fz : (k + 1) * fz] = yo[k]
        square = square + jnp.sum(yov[k] * yov[k], axis=1, keepdims=True)
    rs2 = lax.rsqrt(square * (1.0 / (nr * fb)) + EPS)
    lane = lax.broadcasted_iota(jnp.int32, (td, LANES), 1)
    ids = expert_ids[...].astype(f32)
    ida, idb = ids[:, 0:1], ids[:, 1:2]
    about = jnp.where(lane == 0, rs2, jnp.where(lane == 1, ida, idb))
    for e in range(2):
        names = jnp.where((ida == e) | (idb == e), 1.0, 0.0)
        before = [jnp.zeros((1, 1), f32)]
        for k in range(1, td):
            before.append(before[-1] + names[k - 1 : k, :])
        want = jnp.where(names > 0.0, e * CAPACITY + jnp.concatenate(before, axis=0), -1.0)
        about = jnp.where(lane == 3 + e, want, about)
    info_s[...] = about
    send("tp", "info", lambda p: info_s, info_r)

    for k in range(nx):
        arrived("ez%d" % k, pez.at[k])
        done = total(pez.at[k]).astype(bf16)
        if k == 0:
            fin[pl.ds(x, 1)] = done[None]
        else:
            fin_s[k] = done
            remote(fin_s.at[k], fin.at[x], PH["fin"], {"rep_1": (x + nx - k) % nx})

    arrived("info", info_r)
    arrived("lz", lgz)
    inf = info_r[...].reshape(rq, LANES)
    scale = inf[:, 0:1]
    id0, id1 = inf[:, 1:2], inf[:, 2:3]
    logits = total(lgz) * scale
    lane = lax.broadcasted_iota(jnp.int32, (rq, LANES), 1).astype(f32)
    zero = jnp.zeros((), f32)
    first = jnp.sum(jnp.where(lane == id0, logits, zero), axis=1, keepdims=True)
    second = jnp.sum(jnp.where(lane == id1, logits, zero), axis=1, keepdims=True)
    gate_first = sigmoid(first - second)
    gate_second = sigmoid(second - first)
    inft = inf.T
    slots = 2 * CAPACITY * nt
    slot = lax.broadcasted_iota(jnp.int32, (slots, rq), 0).astype(f32)
    token_at = lax.broadcasted_iota(jnp.int32, (slots, rq), 1)
    base = ((token_at // td) * (2 * CAPACITY)).astype(f32)
    others = fin.at[pl.ds(0, nx - 1)]
    if nx > 1:
        arrived("fin", others)
        pending.append((PH["fin"], others))
    result = jnp.zeros((slots, hid), f32)
    for e in range(2):
        gate = jnp.where(id0 == e, gate_first, zero) + jnp.where(id1 == e, gate_second, zero)
        gate = gate.astype(bf16).astype(f32)
        halves = []
        for j in range(2):
            q = 2 * e + j
            halves.append(fin[q // per_x, q % per_x].astype(f32) * scale)
        hidden = (gate * silu(halves[0]) * halves[1]).astype(bf16)
        want = inft[3 + e : 4 + e, :]
        pick = jnp.where((slot == base + want) & (want >= 0.0), 1.0, 0.0).astype(bf16)
        result = result + dot(pick, hidden)
    expert_hidden[...] = result.astype(bf16)

    for k, part in pending:
        pltpu.make_async_copy(part, part, ssem.at[k]).wait()


def shards(
    nz, nx, nt, tokens, conv_state, ssm_state, norm_gains, conv_weight, conv_skip, step_bias, decay_log,
    input_proj, select_proj, step_proj, output_proj, router, expert_proj, expert_ids,
):
    nr = nz * nx
    rows = input_proj.shape[0]
    td, model = tokens.shape
    rq = td * nt
    fb = rows * nt
    fz = fb * nx
    _, st, ch = ssm_state.shape
    hid = expert_proj.shape[3] // nt
    width = select_proj.shape[1]
    srw = -(-width // 8) * 8
    sp = -(-width * nr // LANES) * LANES
    prw = -(-(7 + st) // 8) * 8
    per_x = 4 // nx
    oc = output_proj.shape[1]

    V = pltpu.VMEM
    scratch = dict(
        x1=((nr, td, fb), bf16), xb=((nz, td, fz), bf16), x2=((nt, nr, td, fb), bf16),
        xx=((nx, nz, rq, fb), bf16),
        rs_s=((td, LANES), f32), rs_r=((nt, td, LANES), f32),
        wi_s=((2 * rows, nt * ch), bf16), wi_r=((nt, 2 * rows, ch), bf16),
        gn_s=((2, LANES), bf16), gn_r=((nt, 2, LANES), bf16), gn_b=((2, fb), bf16), gn_x=((nx, 2, fb), bf16),
        rg_s=((rows, LANES), bf16), rg_r=((nt, rows, LANES), bf16), rg_x=((nx, nt, rows, LANES), bf16),
        wo_r=((nt, oc, ch), bf16), wo_x=((nx, nt, oc, ch), bf16),
        st_s=((nt, nt * ch), bf16), st_r=((nt, nt, ch), bf16), st_b=((nt, ch), bf16),
        st_z=((nz, nt, ch), bf16), st_x=((nx, nz, nt, ch), bf16),
        pk=((prw, LANES), f32), pr_s=((prw, LANES), bf16), pr_z=((nz, prw, LANES), bf16),
        pr_x=((nx, nz, prw, LANES), bf16), pr2=((nt, prw, LANES), bf16),
        se_s=((srw, ch), bf16), se_z=((nz, srw, ch), bf16), se_x=((nx, nz, srw, ch), bf16),
        p3=((nx, nz, rq, 2 * ch), bf16), p3x=((nx, nz, rq, 2 * ch), bf16),
        p3zs=((nz, rq, 2 * ch), bf16), p3z=((nz, rq, 2 * ch), bf16),
        we_s=((4, rows, nt * hid), bf16), we_r=((4, nt, rows, hid), bf16), we_x=((nx, per_x, nt, rows, hid), bf16),
        sel_s=((rq, sp), bf16), sel_r=((nt, rq, sp), bf16),
        maps=((rq, 2 * st, LANES), f32), step_b=((rq, ch), f32), act_b=((rq, ch), f32),
        ro_b=((rq, ch), f32),
        ga_s=((rq, ch), bf16), g_z=((nz, rq, ch), bf16),
        mo_s=((nz, nt, td, fz), bf16), mc_r=((nt, nz, td, fz), bf16), y_s=((nz, td, fz), bf16),
        y2=((nt, nz, td, fz), bf16), yo=((nz, td, fz), bf16), yx=((nx, nz, rq, fz), bf16),
        info_s=((td, LANES), f32), info_r=((nt, td, LANES), f32),
        lg=((nz, rq, LANES), bf16), lgz=((nz, rq, LANES), bf16),
        pe=((nx, nz, per_x, rq, hid), bf16), pez=((nx, nz, per_x, rq, hid), bf16),
        fin_s=((nx, per_x, rq, hid), bf16), fin=((nx, per_x, rq, hid), bf16),
    )
    scratch_shapes = [V(s, d) for s, d in scratch.values()]
    scratch_shapes += [pltpu.SemaphoreType.DMA((len(PHASES),))] * 2
    operands = (
        tokens, conv_state, ssm_state, norm_gains, conv_weight, conv_skip, step_bias[None], decay_log,
        input_proj, select_proj.T, step_proj, output_proj.T, router, expert_proj, expert_ids,
    )
    return pl.pallas_call(
        functools.partial(kernel, nz, nx, nt),
        out_shape=(
            jax.ShapeDtypeStruct((td, model), bf16),
            jax.ShapeDtypeStruct(conv_state.shape, bf16),
            jax.ShapeDtypeStruct(ssm_state.shape, f32),
            jax.ShapeDtypeStruct((2 * CAPACITY * nt, hid), bf16),
        ),
        in_specs=[pl.BlockSpec(memory_space=V)] * len(operands),
        out_specs=[pl.BlockSpec(memory_space=V)] * 4,
        scratch_shapes=scratch_shapes,
        compiler_params=pltpu.CompilerParams(
            collective_id=0, has_side_effects=True, vmem_limit_bytes=60 * 1024 * 1024
        ),
        name="step",
    )(*operands)


def solution(mesh, nz=4):
    devices = mesh.devices
    nx, nt = devices.shape[0] // nz, devices.shape[1]
    split = Mesh(devices.reshape(nz, nx, nt), REP_TP)
    return jax.shard_map(
        functools.partial(shards, nz, nx, nt),
        mesh=split,
        in_specs=(
            P(REP_TP, None),
            P(None, REP, "tp"),
            P(REP, None, "tp"),
            P(None, REP_TP),
            P(None, REP_TP),
            P(None, REP_TP),
            P(REP_TP),
            P(None, REP_TP),
            P(REP_TP, None, None),
            P("tp", REP),
            P(REP_TP, None),
            P(None, REP_TP),
            P(REP_TP, None),
            P(REP_TP, None, None, None),
            P(REP_TP, None),
        ),
        out_specs=(P(REP_TP, None), P(None, REP, "tp"), P(REP, None, "tp"), P(REP, "tp")),
        check_vma=False,
    )
```

```python
import functools

import jax
import jax.numpy as jnp
from jax import lax
from jax.experimental import pallas as pl
from jax.experimental.pallas import tpu as pltpu
from jax.sharding import Mesh
from jax.sharding import PartitionSpec as P

CAPACITY = 2
REP = ("rep_0", "rep_1")
REP_TP = ("rep_0", "rep_1", "tp")
MESH = pl.DeviceIdType.MESH
EPS = 1e-05
bf16 = jnp.bfloat16
f32 = jnp.float32
LANES = 128

PHASES = (
    "x1", "xb", "rs", "wi0", "wi1", "gn", "rg", "prz", "sez", "x2",
    "st", "wo", "we0", "we1", "stz", "p3x0", "p3x1", "p3z0", "p3z1", "prx",
    "sex", "pr2", "stx", "gnx", "rgx", "wox", "wex", "sel", "gz", "mc",
    "y2", "yo", "info", "lz", "ysx", "y2b", "yx1", "yx2", "yx3", "ez0",
    "ez1", "ez2", "ez3", "fin",
)
PH = {name: k for k, name in enumerate(PHASES)}


def sigmoid(v):
    return 1.0 / (1.0 + jnp.exp(-v))


def silu(v):
    return v / (1.0 + jnp.exp(-v))


def softplus(v):
    return jnp.maximum(v, 0.0) + jnp.log1p(jnp.exp(-jnp.abs(v)))


def dot(a, b):
    return jnp.dot(a, b, preferred_element_type=f32)


def dot_nt(a, b):
    return lax.dot_general(a, b, (((1,), (1,)), ((), ())), preferred_element_type=f32)


def write_out(*refs):
    copies = [pltpu.make_async_copy(refs[k], refs[4 + k], refs[8].at[k]) for k in range(4)]
    for copy in copies:
        copy.start()
    for copy in copies:
        copy.wait()


def kernel(
    nz, nx, nt,
    tokens, norm_gains, conv_weight, conv_skip, step_bias, decay_log, step_row, router, expert_ids,
    input_hbm, select_hbm, output_hbm, expert_hbm, conv_hbm, ssm_hbm,
    mamba_out, conv_next, ssm_next, expert_hidden,
    input_proj, select_t, output_t, expert_proj, conv_state, ssm_state,
    x1, xb, x2, xx, rs_s, rs_r, wi_s, wi_r, gn_s, gn_r, gn_b, gn_x, rg_s, rg_r, rg_b, rg_x, wo_r, wo_x,
    st_s, st_r, st_b, st_z, st_x, pk, pr_s, pr_z, pr_x, pr2, se_s, se_z, se_x, p3, p3x, p3zs, p3z,
    we_s, we_r, we_x, sel_s, sel_r, maps, step_b, act_b, ro_b, ga_s, g_z,
    mo_s, mc_r, y_s, y2, ysx, y2b, yo, yx, info_s, info_r, lg, lgz, pe, pez, fin_s, fin,
    ssem, rsem, lsem,
):
    nr = nz * nx
    z, x, t = lax.axis_index("rep_0"), lax.axis_index("rep_1"), lax.axis_index("tp")
    r = z * nx + x
    rows = input_proj.shape[0]
    fb = rows * nt
    fz = fb * nx
    ch = ssm_state.shape[2]
    st = ssm_state.shape[1]
    td = tokens.shape[0]
    rq = td * nt
    rank = nr * nt
    hid = expert_proj.shape[3] // nt
    cdev = conv_weight.shape[1]
    per_x = 4 // nx
    groups = {
        "tp": (nt, t, lambda p: {"tp": p}),
        "rep": (nr, r, lambda p: {"rep_0": p // nx, "rep_1": p % nx}),
        "x": (nx, x, lambda p: {"rep_1": p}),
        "z": (nz, z, lambda p: {"rep_0": p}),
    }
    pending = []

    def remote(src, dst, k, device):
        pltpu.make_async_remote_copy(
            src_ref=src, dst_ref=dst, send_sem=ssem.at[k], recv_sem=rsem.at[k],
            device_id=device, device_id_type=MESH,
        ).start()

    def send(group, name, src, dst, at=None, part=None):
        n, me, dev = groups[group]
        k = PH[name]
        at = at or (lambda me: dst.at[me])

        def body(step, carry):
            peer = (me + step) % n
            remote(src(peer), at(me), k, dev(peer))
            return carry

        if n > 1:
            lax.fori_loop(1, n, body, 0)
            pending.append((k, dst.at[pl.ds(0, n - 1)] if part is None else part))
        pltpu.make_async_copy(src(me), at(me), rsem.at[k]).start()

    def arrived(name, dst):
        pltpu.make_async_copy(dst, dst, rsem.at[PH[name]]).wait()

    def cols(ref, p, width):
        return ref.at[:, pl.ds(pl.multiple_of(p * width, width), width)]

    def total(ref):
        acc = ref[0].astype(f32)
        for k in range(1, ref.shape[0]):
            acc = acc + ref[k].astype(f32)
        return acc

    barrier = pltpu.get_barrier_semaphore()
    for group in ("tp", "rep"):
        n, me, dev = groups[group]

        def greet(step, carry, n=n, me=me, dev=dev):
            pl.semaphore_signal(barrier, inc=1, device_id=dev((me + step) % n), device_id_type=MESH)
            return carry

        lax.fori_loop(1, n, greet, 0)

    loads = {}
    for k, (name, src, dst) in enumerate((
        ("input", input_hbm, input_proj), ("select", select_hbm, select_t), ("output", output_hbm, output_t),
        ("expert", expert_hbm, expert_proj), ("conv", conv_hbm, conv_state), ("ssm", ssm_hbm, ssm_state),
    )):
        loads[name] = pltpu.make_async_copy(src, dst, lsem.at[k])
        loads[name].start()

    gn_s[...] = jnp.zeros(gn_s.shape, bf16)
    gn_s[:, 0:rows] = norm_gains[...]
    loads["input"].wait()
    pl.semaphore_wait(barrier, nt - 1 + nr - 1)
    send("rep", "x1", lambda p: cols(tokens, p, fb), x1)
    send("tp", "gn", lambda p: gn_s, gn_r)
    for j in range(2):
        wi_s[j] = input_proj[:, j, :]
        send("tp", "wi%d" % j, lambda p, j=j: cols(wi_s.at[j], p, ch), wi_r.at[j])
    pk[...] = jnp.zeros(pk.shape, f32)
    pk[0:4, 0:cdev] = conv_weight[...].astype(f32)
    pk[4:6, 0:cdev] = conv_skip[...].astype(f32)
    pk[6:7, 0:cdev] = step_bias[...].astype(f32)
    pk[7 : 7 + st, 0:cdev] = decay_log[...].astype(f32)
    pr_s[...] = pk[...].astype(bf16)
    send("z", "prz", lambda p: pr_s, pr_z)
    se_s[...] = jnp.zeros(se_s.shape, bf16)
    loads["select"].wait()
    se_s[0 : select_t.shape[0], :] = select_t[...]
    send("z", "sez", lambda p: se_s, se_z)
    send("z", "xb", lambda p: cols(tokens, p, fz), xb)
    at_row = lax.broadcasted_iota(jnp.int32, (nt, 1), 0) == t
    st_s[...] = jnp.where(at_row, step_row[...].astype(f32), 0.0).astype(bf16)
    arrived("x1", x1)
    send("tp", "x2", lambda p: x1, x2)
    send("tp", "st", lambda p: cols(st_s, p, ch), st_r)
    xf = tokens[...].astype(f32)
    rs = lax.rsqrt(jnp.mean(xf * xf, axis=1, keepdims=True) + EPS)
    rs_s[...] = jnp.broadcast_to(rs, (td, LANES))
    send("tp", "rs", lambda p: rs_s, rs_r)
    rg_s[...] = jnp.zeros(rg_s.shape, bf16)
    rg_s[:, 0 : router.shape[1]] = router[...]
    send("tp", "rg", lambda p: rg_s, rg_r)

    def send_experts(e):
        for j in range(2):
            we_s[2 * e + j] = expert_proj[:, e, j, :]
        half = we_r.at[pl.ds(2 * e, 2)]
        send(
            "tp", "we%d" % e,
            lambda p: we_s.at[pl.ds(2 * e, 2), :, pl.ds(pl.multiple_of(p * hid, hid), hid)], half,
            at=lambda me: half.at[:, me], part=half.at[:, pl.ds(0, nt - 1)],
        )

    arrived("prz", pr_z)
    send("x", "prx", lambda p: pr_z, pr_x)
    arrived("gn", gn_r)
    gnv = gn_r[...].astype(f32)
    gains = jnp.concatenate([gnv[k][:, 0:rows] for k in range(nt)], axis=1)
    gn_b[...] = gains.astype(bf16)
    gain0 = gains[0:1, :]
    arrived("x2", x2)

    def place_in(q, carry):
        block = x2[:, q].reshape(rq, fb).astype(f32)
        xx[q % nx, q // nx] = (block * gain0).astype(bf16)
        return carry

    lax.fori_loop(0, nr, place_in, 0)
    lhs = xx[...].reshape(nr * rq, fb)

    def partial_in(j):
        arrived("wi%d" % j, wi_r.at[j])
        p3[j] = dot(lhs, wi_r[j].reshape(fb, ch)).astype(bf16).reshape(nx, nz, rq, ch)

    def send_in(j):
        send("x", "p3x%d" % j, lambda p: p3.at[j, p], p3x.at[j])

    def sum_in(j):
        arrived("p3x%d" % j, p3x.at[j])
        p3zs[j] = total(p3x.at[j]).astype(bf16)
        send("z", "p3z%d" % j, lambda p: p3zs.at[j, p], p3z.at[j])

    partial_in(0)
    send_in(0)

    arrived("st", st_r)
    st_b[...] = jnp.sum(st_r[...].astype(f32), axis=0).astype(bf16)
    send("z", "stz", lambda p: st_b, st_z)
    arrived("sez", se_z)
    send("x", "sex", lambda p: se_z, se_x)
    partial_in(1)
    arrived("prx", pr_x)
    send("tp", "pr2", lambda p: pr_x.at[p % nx, p // nx], pr2)
    loads["output"].wait()
    send("tp", "wo", lambda p: cols(output_t, p, ch), wo_r)
    loads["expert"].wait()
    send_experts(0)
    arrived("stz", st_z)
    send("x", "stx", lambda p: st_z, st_x)
    send_in(1)
    sum_in(0)
    send_experts(1)
    arrived("rg", rg_r)
    rgt = rg_r[...].reshape(fb, LANES).astype(f32).T
    rg_b[...] = rgt[0 : rg_b.shape[0]].astype(bf16)
    send("x", "gnx", lambda p: gn_b, gn_x)
    send("x", "rgx", lambda p: rg_b, rg_x)
    arrived("wo", wo_r)
    send("x", "wox", lambda p: wo_r, wo_x)
    arrived("sex", se_x)
    srw = se_s.shape[0]
    sp = sel_s.shape[1]
    width = select_t.shape[0]
    shape = (sp, nr * srw)
    at_col = lax.broadcasted_iota(jnp.int32, shape, 0)
    place_of = lax.broadcasted_iota(jnp.int32, shape, 1)
    blk, off = place_of // srw, place_of % srw
    true_col = ((blk % nz) * nx + blk // nz) * width + off
    perm = jnp.where((true_col == at_col) & (off < width), 1.0, 0.0).astype(bf16)
    select_all = dot(perm, se_x[...].reshape(nr * srw, ch)).astype(bf16)
    arrived("rs", rs_r)
    rsv = rs_r[...].reshape(rq, LANES)[:, 0:1]
    arrived("pr2", pr2)
    prv = pr2[...].astype(f32)
    par = jnp.concatenate([prv[k][:, 0:cdev] for k in range(nt)], axis=1)
    loads["conv"].wait()
    history = jnp.sum(par[0:3][:, None, :] * conv_state[...].astype(f32), axis=0) + par[4:5]
    decay_rate = -jnp.exp(par[7 : 7 + st])
    conv_next[0] = conv_state[1]
    conv_next[1] = conv_state[2]
    arrived("p3z0", p3z.at[0])
    conv_input = total(p3z.at[0]) * rsv
    conv_next[2] = conv_input.astype(bf16)
    activated = silu(history + par[3:4] * conv_input)
    sel_s[...] = dot_nt(activated.astype(bf16), select_all).astype(bf16)
    send("tp", "sel", lambda p: sel_s, sel_r)
    act_b[...] = activated
    sum_in(1)
    for e in range(2):
        arrived("we%d" % e, we_r.at[pl.ds(2 * e, 2)])
    send("x", "wex", lambda p: we_r.at[pl.ds(p * per_x, per_x)], we_x)
    loads["ssm"].wait()
    arrived("stx", st_x)
    step_all = jnp.concatenate([st_x[q % nx, q // nx] for q in range(nr)], axis=0)
    arrived("sel", sel_r)
    selected = total(sel_r)
    step_low = selected[:, :rank].astype(bf16)
    maps[...] = jnp.broadcast_to(selected[:, rank : rank + 2 * st][:, :, None], maps.shape)
    step_b[...] = softplus(dot(step_low, step_all) + par[6:7])

    def token(i, carry):
        s = step_b[pl.ds(i, 1), :]
        a = act_b[pl.ds(i, 1), :]
        m = maps[i]
        wide = jnp.concatenate([m] * (ch // LANES), axis=1)
        nxt = jnp.exp(s * decay_rate) * ssm_state[i] + (s * a) * wide[:st]
        ssm_next[i] = nxt
        ro_b[pl.ds(i, 1), :] = jnp.sum(nxt * wide[st:], axis=0, keepdims=True)
        return carry

    lax.fori_loop(0, rq, token, 0)
    readout = ro_b[...] + par[5:6] * activated
    arrived("p3z1", p3z.at[1])
    gate_z = total(p3z.at[1]) * rsv
    ga_s[...] = (readout * silu(gate_z)).astype(bf16)

    send("z", "gz", lambda p: ga_s, g_z)
    arrived("wox", wo_x)
    arrived("gz", g_z)
    mo = dot_nt(g_z[...].reshape(nz * rq, ch), wo_x[...].reshape(fz, ch))
    mo_s[...] = mo.astype(bf16).reshape(nz, nt, td, fz)
    send("tp", "mc", lambda p: mo_s.at[:, p], mc_r)
    arrived("xb", xb)
    arrived("mc", mc_r)
    y_s[...] = (xb[...].astype(f32) + total(mc_r)).astype(bf16)
    relay = nx // 2 if nx > 2 else 0
    if relay:
        remote(y_s, ysx, PH["ysx"], {"rep_1": (x + relay) % nx})
        pending.append((PH["ysx"], ysx))
    send("tp", "y2", lambda p: y_s, y2)
    send("z", "yo", lambda p: y_s.at[p], yo)

    arrived("gnx", gn_x)
    gain1 = jnp.concatenate([gn_x[k].astype(f32)[1:2, :] for k in range(nx)], axis=1)
    arrived("rgx", rg_x)
    experts = rg_b.shape[0]
    router_all = jnp.concatenate([rg_x[k] for k in range(nx)], axis=1)
    if relay:
        arrived("ysx", ysx)
        send("tp", "y2b", lambda p: ysx, y2b)

    def place_out(src, k):
        for q in range(nz):
            block = src[:, q].reshape(rq, fz).astype(f32)
            yx[k, q] = (block * gain1).astype(bf16)

    arrived("y2", y2)
    place_out(y2, 0)
    for k in range(1, nx):
        if k != relay:
            remote(yx.at[0], yx.at[k], PH["yx%d" % k], {"rep_1": (x + k) % nx})
            pending.append((PH["yx%d" % k], yx.at[0]))
    arrived("wex", we_x)
    order = [0] + ([relay] if relay else []) + [k for k in range(1, nx) if k != relay]
    for k in order:
        if relay and k == relay:
            arrived("y2b", y2b)
            place_out(y2b, k)
        elif k:
            arrived("yx%d" % k, yx.at[k])
        left = yx[k].reshape(nz * rq, fz)
        for c in range(per_x):
            part = dot(left, we_x[:, c].reshape(fz, hid))
            pe[k, :, c] = part.astype(bf16).reshape(nz, rq, hid)
        send("z", "ez%d" % k, lambda p, k=k: pe.at[k, p], pez.at[k])
        if k == 0:
            lg[:, :, 0:experts] = dot_nt(left, router_all).astype(bf16).reshape(nz, rq, experts)
            send("z", "lz", lambda p: lg.at[p], lgz)

    arrived("yo", yo)
    yov = [yo[k].astype(f32) for k in range(nz)]
    square = jnp.zeros((td, 1), f32)
    for k in range(nz):
        mamba_out[:, k * fz : (k + 1) * fz] = yo[k]
        square = square + jnp.sum(yov[k] * yov[k], axis=1, keepdims=True)
    rs2 = lax.rsqrt(square * (1.0 / (nr * fb)) + EPS)
    lane = lax.broadcasted_iota(jnp.int32, (td, LANES), 1)
    ids = expert_ids[...].astype(f32)
    ida, idb = ids[:, 0:1], ids[:, 1:2]
    about = jnp.where(lane == 0, rs2, jnp.where(lane == 1, ida, idb))
    for e in range(2):
        names = jnp.where((ida == e) | (idb == e), 1.0, 0.0)
        before = [jnp.zeros((1, 1), f32)]
        for k in range(1, td):
            before.append(before[-1] + names[k - 1 : k, :])
        want = jnp.where(names > 0.0, e * CAPACITY + jnp.concatenate(before, axis=0), -1.0)
        about = jnp.where(lane == 3 + e, want, about)
    info_s[...] = about
    send("tp", "info", lambda p: info_s, info_r)

    for k in order:
        arrived("ez%d" % k, pez.at[k])
        done = total(pez.at[k]).astype(bf16)
        if k == 0:
            fin[pl.ds(x, 1)] = done[None]
        else:
            fin_s[k] = done
            remote(fin_s.at[k], fin.at[x], PH["fin"], {"rep_1": (x + nx - k) % nx})

    arrived("info", info_r)
    arrived("lz", lgz)
    inf = info_r[...].reshape(rq, LANES)
    scale = inf[:, 0:1]
    id0, id1 = inf[:, 1:2], inf[:, 2:3]
    logits = (total(lgz) * scale)[:, 0:experts]
    lane = lax.broadcasted_iota(jnp.int32, (rq, experts), 1).astype(f32)
    zero = jnp.zeros((), f32)
    first = jnp.sum(jnp.where(lane == id0, logits, zero), axis=1, keepdims=True)
    second = jnp.sum(jnp.where(lane == id1, logits, zero), axis=1, keepdims=True)
    gate_first = sigmoid(first - second)
    gate_second = sigmoid(second - first)
    inft = inf.T
    slots = 2 * CAPACITY * nt
    slot = lax.broadcasted_iota(jnp.int32, (slots, rq), 0).astype(f32)
    token_at = lax.broadcasted_iota(jnp.int32, (slots, rq), 1)
    base = ((token_at // td) * (2 * CAPACITY)).astype(f32)
    others = fin.at[pl.ds(0, nx - 1)]
    if nx > 1:
        arrived("fin", others)
        pending.append((PH["fin"], others))
    result = jnp.zeros((slots, hid), f32)
    for e in range(2):
        gate = jnp.where(id0 == e, gate_first, zero) + jnp.where(id1 == e, gate_second, zero)
        gate = gate.astype(bf16).astype(f32)
        halves = []
        for j in range(2):
            q = 2 * e + j
            halves.append(fin[q // per_x, q % per_x].astype(f32) * scale)
        hidden = (gate * silu(halves[0]) * halves[1]).astype(bf16)
        want = inft[3 + e : 4 + e, :]
        pick = jnp.where((slot == base + want) & (want >= 0.0), 1.0, 0.0).astype(bf16)
        result = result + dot(pick, hidden)
    expert_hidden[...] = result.astype(bf16)

    for k, part in pending:
        pltpu.make_async_copy(part, part, ssem.at[k]).wait()


def shards(
    nz, nx, nt, tokens, conv_state, ssm_state, norm_gains, conv_weight, conv_skip, step_bias, decay_log,
    input_proj, select_proj, step_proj, output_proj, router, expert_proj, expert_ids,
):
    nr = nz * nx
    rows = input_proj.shape[0]
    td, model = tokens.shape
    rq = td * nt
    fb = rows * nt
    fz = fb * nx
    _, st, ch = ssm_state.shape
    hid = expert_proj.shape[3] // nt
    width = select_proj.shape[1]
    srw = -(-width // 8) * 8
    sp = -(-width * nr // LANES) * LANES
    prw = -(-(7 + st) // 8) * 8
    per_x = 4 // nx
    oc = output_proj.shape[1]

    V = pltpu.VMEM
    experts = router.shape[1]
    small = (
        tokens, norm_gains, conv_weight, conv_skip, step_bias[None], decay_log, step_proj, router, expert_ids,
    )
    large = (input_proj, select_proj.T, output_proj.T, expert_proj, conv_state, ssm_state)
    scratch = {"load%d" % k: (a.shape, a.dtype) for k, a in enumerate(large)}
    scratch.update(
        x1=((nr, td, fb), bf16), xb=((nz, td, fz), bf16), x2=((nt, nr, td, fb), bf16),
        xx=((nx, nz, rq, fb), bf16),
        rs_s=((td, LANES), f32), rs_r=((nt, td, LANES), f32),
        wi_s=((2, rows, nt * ch), bf16), wi_r=((2, nt, rows, ch), bf16),
        gn_s=((2, LANES), bf16), gn_r=((nt, 2, LANES), bf16), gn_b=((2, fb), bf16), gn_x=((nx, 2, fb), bf16),
        rg_s=((rows, LANES), bf16), rg_r=((nt, rows, LANES), bf16), rg_b=((experts, fb), bf16),
        rg_x=((nx, experts, fb), bf16),
        wo_r=((nt, oc, ch), bf16), wo_x=((nx, nt, oc, ch), bf16),
        st_s=((nt, nt * ch), bf16), st_r=((nt, nt, ch), bf16), st_b=((nt, ch), bf16),
        st_z=((nz, nt, ch), bf16), st_x=((nx, nz, nt, ch), bf16),
        pk=((prw, LANES), f32), pr_s=((prw, LANES), bf16), pr_z=((nz, prw, LANES), bf16),
        pr_x=((nx, nz, prw, LANES), bf16), pr2=((nt, prw, LANES), bf16),
        se_s=((srw, ch), bf16), se_z=((nz, srw, ch), bf16), se_x=((nx, nz, srw, ch), bf16),
        p3=((2, nx, nz, rq, ch), bf16), p3x=((2, nx, nz, rq, ch), bf16),
        p3zs=((2, nz, rq, ch), bf16), p3z=((2, nz, rq, ch), bf16),
        we_s=((4, rows, nt * hid), bf16), we_r=((4, nt, rows, hid), bf16), we_x=((nx, per_x, nt, rows, hid), bf16),
        sel_s=((rq, sp), bf16), sel_r=((nt, rq, sp), bf16),
        maps=((rq, 2 * st, LANES), f32), step_b=((rq, ch), f32), act_b=((rq, ch), f32),
        ro_b=((rq, ch), f32),
        ga_s=((rq, ch), bf16), g_z=((nz, rq, ch), bf16),
        mo_s=((nz, nt, td, fz), bf16), mc_r=((nt, nz, td, fz), bf16), y_s=((nz, td, fz), bf16),
        y2=((nt, nz, td, fz), bf16), ysx=((nz, td, fz), bf16), y2b=((nt, nz, td, fz), bf16), yo=((nz, td, fz), bf16), yx=((nx, nz, rq, fz), bf16),
        info_s=((td, LANES), f32), info_r=((nt, td, LANES), f32),
        lg=((nz, rq, LANES), bf16), lgz=((nz, rq, LANES), bf16),
        pe=((nx, nz, per_x, rq, hid), bf16), pez=((nx, nz, per_x, rq, hid), bf16),
        fin_s=((nx, per_x, rq, hid), bf16), fin=((nx, per_x, rq, hid), bf16),
    )
    scratch_shapes = [V(s, d) for s, d in scratch.values()]
    scratch_shapes += [pltpu.SemaphoreType.DMA((len(PHASES),))] * 2 + [pltpu.SemaphoreType.DMA((len(large),))]
    outs = (
        ((td, model), bf16), (conv_state.shape, bf16), (ssm_state.shape, f32),
        ((2 * CAPACITY * nt, hid), bf16),
    )
    results = pl.pallas_call(
        functools.partial(kernel, nz, nx, nt),
        out_shape=tuple(V(s, d) for s, d in outs),
        in_specs=[pl.BlockSpec(memory_space=V)] * len(small) + [pl.BlockSpec(memory_space=pl.ANY)] * len(large),
        out_specs=[pl.BlockSpec(memory_space=V)] * 4,
        scratch_shapes=scratch_shapes,
        compiler_params=pltpu.CompilerParams(
            collective_id=0, has_side_effects=True, vmem_limit_bytes=61 * 1024 * 1024
        ),
        name="step",
    )(*small, *large)
    results = [pltpu.with_memory_space_constraint(a, V) for a in results]
    return pl.pallas_call(
        write_out,
        out_shape=tuple(jax.ShapeDtypeStruct(s, d) for s, d in outs),
        in_specs=[pl.BlockSpec(memory_space=V)] * 4,
        out_specs=[pl.BlockSpec(memory_space=pl.ANY)] * 4,
        scratch_shapes=[pltpu.SemaphoreType.DMA((4,))],
        name="write_out",
    )(*results)


def solution(mesh, nz=4):
    devices = mesh.devices
    nx, nt = devices.shape[0] // nz, devices.shape[1]
    split = Mesh(devices.reshape(nz, nx, nt), REP_TP)
    return jax.shard_map(
        functools.partial(shards, nz, nx, nt),
        mesh=split,
        in_specs=(
            P(REP_TP, None),
            P(None, REP, "tp"),
            P(REP, None, "tp"),
            P(None, REP_TP),
            P(None, REP_TP),
            P(None, REP_TP),
            P(REP_TP),
            P(None, REP_TP),
            P(REP_TP, None, None),
            P("tp", REP),
            P(REP_TP, None),
            P(None, REP_TP),
            P(REP_TP, None),
            P(REP_TP, None, None, None),
            P(REP_TP, None),
        ),
        out_specs=(P(REP_TP, None), P(None, REP, "tp"), P(REP, None, "tp"), P(REP, "tp")),
        check_vma=False,
    )
```

```python
import functools

import jax
import jax.numpy as jnp
from jax import lax
from jax.experimental import pallas as pl
from jax.experimental.pallas import tpu as pltpu
from jax.sharding import Mesh
from jax.sharding import PartitionSpec as P

CAPACITY = 2
REP = ("rep_0", "rep_1")
REP_TP = ("rep_0", "rep_1", "tp")
MESH = pl.DeviceIdType.MESH
EPS = 1e-05
bf16 = jnp.bfloat16
f32 = jnp.float32
LANES = 128

PHASES = (
    "x1", "xb", "rs", "wi0", "wi1", "gn", "rg", "prz", "sez", "x2",
    "st", "wo", "we0", "we1", "we2", "stz", "p3x0", "p3x1", "p3z0", "p3z1", "prx",
    "sex", "pr2", "stx", "gnx", "rgx", "wox", "wex0", "wex1", "wex2", "sel", "gz", "mc",
    "y2", "yo", "info", "lz", "ysx", "y2b", "yx1", "yx2", "yx3", "ez0",
    "ez1", "ez2", "ez3", "fin",
)
PH = {name: k for k, name in enumerate(PHASES)}


def sigmoid(v):
    return 1.0 / (1.0 + jnp.exp(-v))


def silu(v):
    return v / (1.0 + jnp.exp(-v))


def softplus(v):
    return jnp.maximum(v, 0.0) + jnp.log1p(jnp.exp(-jnp.abs(v)))


def dot(a, b):
    return jnp.dot(a, b, preferred_element_type=f32)


def dot_nt(a, b):
    return lax.dot_general(a, b, (((1,), (1,)), ((), ())), preferred_element_type=f32)


def write_out(*refs):
    copies = [pltpu.make_async_copy(refs[k], refs[4 + k], refs[8].at[k]) for k in range(4)]
    for copy in copies:
        copy.start()
    for copy in copies:
        copy.wait()


def kernel(
    nz, nx, nt,
    tokens, norm_gains, conv_weight, conv_skip, step_bias, decay_log, step_row, router, expert_ids,
    input_hbm, select_hbm, output_hbm, expert_hbm, conv_hbm, ssm_hbm,
    mamba_out, conv_next, ssm_next, expert_hidden,
    input_proj, select_t, output_t, expert_proj, conv_state, ssm_state,
    x1, xb, x2, xx, rs_s, rs_r, wi_s, wi_r, gn_s, gn_r, gn_b, gn_x, rg_s, rg_r, rg_b, rg_x, wo_r, wo_x,
    st_r, st_b, st_z, st_x, pk, pr_s, pr_z, pr_x, pr2, se_s, se_z, se_x, p3, p3x, p3zs, p3z,
    we_s, we_r, we_x, sel_s, sel_r, maps, step_b, act_b, ro_b, ga_s, g_z,
    mo_s, mc_r, y_s, y2, ysx, y2b, yo, yx, info_s, info_r, lg, lgz, pe, pez, fin_s, fin,
    ssem, rsem, lsem,
):
    nr = nz * nx
    z, x, t = lax.axis_index("rep_0"), lax.axis_index("rep_1"), lax.axis_index("tp")
    r = z * nx + x
    rows = input_proj.shape[0]
    fb = rows * nt
    fz = fb * nx
    ch = ssm_state.shape[2]
    st = ssm_state.shape[1]
    td = tokens.shape[0]
    rq = td * nt
    rank = nr * nt
    hid = expert_proj.shape[3] // nt
    pieces, hc = we_r.shape[0], we_r.shape[4]
    cdev = conv_weight.shape[1]
    per_x = 4 // nx
    groups = {
        "tp": (nt, t, lambda p: {"tp": p}),
        "rep": (nr, r, lambda p: {"rep_0": p // nx, "rep_1": p % nx}),
        "x": (nx, x, lambda p: {"rep_1": p}),
        "z": (nz, z, lambda p: {"rep_0": p}),
    }
    pending = []

    def remote(src, dst, k, device):
        pltpu.make_async_remote_copy(
            src_ref=src, dst_ref=dst, send_sem=ssem.at[k], recv_sem=rsem.at[k],
            device_id=device, device_id_type=MESH,
        ).start()

    def send(group, name, src, dst, at=None, part=None):
        n, me, dev = groups[group]
        k = PH[name]
        at = at or (lambda me: dst.at[me])

        def body(step, carry):
            peer = (me + step) % n
            remote(src(peer), at(me), k, dev(peer))
            return carry

        if n > 1:
            lax.fori_loop(1, n, body, 0)
            pending.append((k, dst.at[pl.ds(0, n - 1)] if part is None else part))
        pltpu.make_async_copy(src(me), at(me), rsem.at[k]).start()

    def arrived(name, dst):
        pltpu.make_async_copy(dst, dst, rsem.at[PH[name]]).wait()

    def cols(ref, p, width):
        return ref.at[:, pl.ds(pl.multiple_of(p * width, width), width)]

    def total(ref):
        acc = ref[0].astype(f32)
        for k in range(1, ref.shape[0]):
            acc = acc + ref[k].astype(f32)
        return acc

    barrier = pltpu.get_barrier_semaphore()
    for group in ("tp", "rep"):
        n, me, dev = groups[group]

        def greet(step, carry, n=n, me=me, dev=dev):
            pl.semaphore_signal(barrier, inc=1, device_id=dev((me + step) % n), device_id_type=MESH)
            return carry

        lax.fori_loop(1, n, greet, 0)

    loads = {}
    for k, (name, src, dst) in enumerate((
        ("input", input_hbm, input_proj), ("select", select_hbm, select_t), ("output", output_hbm, output_t),
        ("expert", expert_hbm, expert_proj), ("conv", conv_hbm, conv_state), ("ssm", ssm_hbm, ssm_state),
    )):
        loads[name] = pltpu.make_async_copy(src, dst, lsem.at[k])
        loads[name].start()

    gn_s[...] = jnp.zeros(gn_s.shape, bf16)
    gn_s[:, 0:rows] = norm_gains[...]

    def send_input(j):
        wi_s[j] = input_proj[:, j, :]
        send("tp", "wi%d" % j, lambda p: cols(wi_s.at[j], p, ch), wi_r.at[j])

    def send_experts(e):
        dst = we_r.at[e]
        send(
            "tp", "we%d" % e,
            lambda p: we_s.at[:, :, pl.ds(pl.multiple_of(p * hid + e * hc, hc), hc)], dst,
            at=lambda me: dst.at[:, me], part=dst.at[:, pl.ds(0, nt - 1)],
        )

    def pass_experts(e):
        arrived("we%d" % e, we_r.at[e])
        send("x", "wex%d" % e, lambda p: we_r.at[e, pl.ds(p * per_x, per_x)], we_x.at[e])

    def lay_experts(e):
        for j in range(2):
            we_s[2 * e + j] = expert_proj[:, e, j, :]

    xf = tokens[...].astype(f32)
    rs = lax.rsqrt(jnp.mean(xf * xf, axis=1, keepdims=True) + EPS)
    rs_s[...] = jnp.broadcast_to(rs, (td, LANES))
    pl.semaphore_wait(barrier, nt - 1 + nr - 1)
    send("rep", "x1", lambda p: cols(tokens, p, fb), x1)
    send("tp", "gn", lambda p: gn_s, gn_r)
    send("tp", "rs", lambda p: rs_s, rs_r)
    pk[...] = jnp.zeros(pk.shape, f32)
    pk[0:4, 0:cdev] = conv_weight[...].astype(f32)
    pk[4:6, 0:cdev] = conv_skip[...].astype(f32)
    pk[6:7, 0:cdev] = step_bias[...].astype(f32)
    pk[7 : 7 + st, 0:cdev] = decay_log[...].astype(f32)
    pr_s[...] = pk[...].astype(bf16)
    send("z", "prz", lambda p: pr_s, pr_z)
    se_s[...] = jnp.zeros(se_s.shape, bf16)
    loads["select"].wait()
    se_s[0 : select_t.shape[0], :] = select_t[...]
    send("z", "sez", lambda p: se_s, se_z)
    loads["input"].wait()
    send_input(0)
    rg_s[...] = jnp.zeros(rg_s.shape, bf16)
    rg_s[:, 0 : router.shape[1]] = router[...]
    arrived("x1", x1)
    send("tp", "x2", lambda p: x1, x2)
    send_input(1)
    send("tp", "st", lambda p: cols(step_row, p, ch), st_r)
    loads["output"].wait()
    send("tp", "wo", lambda p: cols(output_t, p, ch), wo_r)
    send("z", "xb", lambda p: cols(tokens, p, fz), xb)
    loads["expert"].wait()
    lay_experts(0)

    arrived("gn", gn_r)
    gnv = gn_r[...].astype(f32)
    gains = jnp.concatenate([gnv[k][:, 0:rows] for k in range(nt)], axis=1)
    gn_b[...] = gains.astype(bf16)
    gain0 = gains[0:1, :]
    arrived("prz", pr_z)
    send("x", "prx", lambda p: pr_z, pr_x)
    arrived("sez", se_z)
    send("x", "sex", lambda p: se_z, se_x)
    arrived("x2", x2)

    def place_in(q, carry):
        block = x2[:, q].reshape(rq, fb).astype(f32)
        xx[q % nx, q // nx] = (block * gain0).astype(bf16)
        return carry

    lax.fori_loop(0, nr, place_in, 0)
    lhs = xx[...].reshape(nr * rq, fb)

    def partial_in(j):
        arrived("wi%d" % j, wi_r.at[j])
        p3[j] = dot(lhs, wi_r[j].reshape(fb, ch)).astype(bf16).reshape(nx, nz, rq, ch)

    def send_in(j):
        send("x", "p3x%d" % j, lambda p: p3.at[j, p], p3x.at[j])

    def sum_in(j):
        arrived("p3x%d" % j, p3x.at[j])
        p3zs[j] = total(p3x.at[j]).astype(bf16)
        send("z", "p3z%d" % j, lambda p: p3zs.at[j, p], p3z.at[j])

    partial_in(0)
    send_in(0)

    arrived("prx", pr_x)
    send("tp", "pr2", lambda p: pr_x.at[p % nx, p // nx], pr2)
    partial_in(1)
    send_in(1)
    arrived("st", st_r)
    st_b[...] = st_r[...].astype(f32).reshape(nt, ch).astype(bf16)
    send("z", "stz", lambda p: st_b, st_z)
    lay_experts(1)
    send_experts(0)
    sum_in(0)
    send("tp", "rg", lambda p: rg_s, rg_r)
    arrived("stz", st_z)
    send("x", "stx", lambda p: st_z, st_x)
    arrived("wo", wo_r)
    send("x", "wox", lambda p: wo_r, wo_x)
    send("x", "gnx", lambda p: gn_b, gn_x)
    sum_in(1)
    arrived("sex", se_x)
    srw = se_s.shape[0]
    sp = sel_s.shape[1]
    width = select_t.shape[0]
    shape = (sp, nr * srw)
    at_col = lax.broadcasted_iota(jnp.int32, shape, 0)
    place_of = lax.broadcasted_iota(jnp.int32, shape, 1)
    blk, off = place_of // srw, place_of % srw
    true_col = ((blk % nz) * nx + blk // nz) * width + off
    perm = jnp.where((true_col == at_col) & (off < width), 1.0, 0.0).astype(bf16)
    select_all = dot(perm, se_x[...].reshape(nr * srw, ch)).astype(bf16)
    arrived("pr2", pr2)
    prv = pr2[...].astype(f32)
    par = jnp.concatenate([prv[k][:, 0:cdev] for k in range(nt)], axis=1)
    loads["conv"].wait()
    history = jnp.sum(par[0:3][:, None, :] * conv_state[...].astype(f32), axis=0) + par[4:5]
    decay_rate = -jnp.exp(par[7 : 7 + st])
    conv_next[0] = conv_state[1]
    conv_next[1] = conv_state[2]
    arrived("rs", rs_r)
    rsv = rs_r[...].reshape(rq, LANES)[:, 0:1]
    arrived("p3z0", p3z.at[0])
    conv_input = total(p3z.at[0]) * rsv
    conv_next[2] = conv_input.astype(bf16)
    activated = silu(history + par[3:4] * conv_input)
    sel_s[...] = dot_nt(activated.astype(bf16), select_all).astype(bf16)
    send("tp", "sel", lambda p: sel_s, sel_r)
    act_b[...] = activated
    if pieces > 1:
        send_experts(1)
    arrived("rg", rg_r)
    rgt = rg_r[...].reshape(fb, LANES).astype(f32).T
    rg_b[...] = rgt[0 : rg_b.shape[0]].astype(bf16)
    send("x", "rgx", lambda p: rg_b, rg_x)
    pass_experts(0)
    loads["ssm"].wait()
    arrived("stx", st_x)
    step_all = jnp.concatenate([st_x[q % nx, q // nx] for q in range(nr)], axis=0)
    arrived("sel", sel_r)
    selected = total(sel_r)
    step_low = selected[:, :rank].astype(bf16)
    maps[...] = jnp.broadcast_to(selected[:, rank : rank + 2 * st][:, :, None], maps.shape)
    step_b[...] = softplus(dot(step_low, step_all) + par[6:7])

    def token(i, carry):
        s = step_b[pl.ds(i, 1), :]
        a = act_b[pl.ds(i, 1), :]
        m = maps[i]
        wide = jnp.concatenate([m] * (ch // LANES), axis=1)
        nxt = jnp.exp(s * decay_rate) * ssm_state[i] + (s * a) * wide[:st]
        ssm_next[i] = nxt
        ro_b[pl.ds(i, 1), :] = jnp.sum(nxt * wide[st:], axis=0, keepdims=True)
        return carry

    lax.fori_loop(0, rq, token, 0)
    readout = ro_b[...] + par[5:6] * activated
    arrived("p3z1", p3z.at[1])
    gate_z = total(p3z.at[1]) * rsv
    ga_s[...] = (readout * silu(gate_z)).astype(bf16)

    send("z", "gz", lambda p: ga_s, g_z)
    for e in range(2, pieces):
        send_experts(e)
    if pieces > 1:
        pass_experts(1)
    arrived("wox", wo_x)
    arrived("gz", g_z)
    mo = dot_nt(g_z[...].reshape(nz * rq, ch), wo_x[...].reshape(fz, ch))
    mo_s[...] = mo.astype(bf16).reshape(nz, nt, td, fz)
    send("tp", "mc", lambda p: mo_s.at[:, p], mc_r)
    for e in range(2, pieces):
        pass_experts(e)
    arrived("xb", xb)
    arrived("mc", mc_r)
    y_s[...] = (xb[...].astype(f32) + total(mc_r)).astype(bf16)
    relay = nx // 2 if nx > 2 else 0
    if relay:
        remote(y_s, ysx, PH["ysx"], {"rep_1": (x + relay) % nx})
        pending.append((PH["ysx"], ysx))
    send("tp", "y2", lambda p: y_s, y2)
    send("z", "yo", lambda p: y_s.at[p], yo)

    arrived("gnx", gn_x)
    gain1 = jnp.concatenate([gn_x[k].astype(f32)[1:2, :] for k in range(nx)], axis=1)
    arrived("rgx", rg_x)
    experts = rg_b.shape[0]
    router_all = jnp.concatenate([rg_x[k] for k in range(nx)], axis=1)

    def place_out(src, k):
        for q in range(nz):
            block = src[:, q].reshape(rq, fz).astype(f32)
            yx[k, q] = (block * gain1).astype(bf16)

    if relay:
        arrived("ysx", ysx)
        send("tp", "y2b", lambda p: ysx, y2b)
    arrived("y2", y2)
    place_out(y2, 0)
    for k in range(1, nx):
        if k != relay:
            remote(yx.at[0], yx.at[k], PH["yx%d" % k], {"rep_1": (x + k) % nx})
            pending.append((PH["yx%d" % k], yx.at[0]))
    for e in range(pieces):
        arrived("wex%d" % e, we_x.at[e])

    def multiply(k):
        left = yx[k].reshape(nz * rq, fz)
        for c in range(per_x):
            for e in range(pieces):
                part = dot(left, we_x[e, :, c].reshape(fz, hc))
                pe[k, :, c, :, e * hc : (e + 1) * hc] = part.astype(bf16).reshape(nz, rq, hc)

    multiply(0)
    send("z", "ez0", lambda p: pe.at[0, p], pez.at[0])
    left = yx[0].reshape(nz * rq, fz)
    lg[:, :, 0:experts] = dot_nt(left, router_all).astype(bf16).reshape(nz, rq, experts)
    send("z", "lz", lambda p: lg.at[p], lgz)

    arrived("yo", yo)
    yov = [yo[k].astype(f32) for k in range(nz)]
    square = jnp.zeros((td, 1), f32)
    for k in range(nz):
        mamba_out[:, k * fz : (k + 1) * fz] = yo[k]
        square = square + jnp.sum(yov[k] * yov[k], axis=1, keepdims=True)
    rs2 = lax.rsqrt(square * (1.0 / (nr * fb)) + EPS)
    lane = lax.broadcasted_iota(jnp.int32, (td, LANES), 1)
    ids = expert_ids[...].astype(f32)
    ida, idb = ids[:, 0:1], ids[:, 1:2]
    about = jnp.where(lane == 0, rs2, jnp.where(lane == 1, ida, idb))
    for e in range(2):
        names = jnp.where((ida == e) | (idb == e), 1.0, 0.0)
        before = [jnp.zeros((1, 1), f32)]
        for k in range(1, td):
            before.append(before[-1] + names[k - 1 : k, :])
        want = jnp.where(names > 0.0, e * CAPACITY + jnp.concatenate(before, axis=0), -1.0)
        about = jnp.where(lane == 3 + e, want, about)
    info_s[...] = about
    send("tp", "info", lambda p: info_s, info_r)

    order = ([relay] if relay else []) + [k for k in range(1, nx) if k != relay]
    for k in order:
        if relay and k == relay:
            arrived("y2b", y2b)
            place_out(y2b, k)
        else:
            arrived("yx%d" % k, yx.at[k])
        multiply(k)
        send("z", "ez%d" % k, lambda p, k=k: pe.at[k, p], pez.at[k])
    for k in order:
        arrived("ez%d" % k, pez.at[k])
        fin_s[k] = total(pez.at[k]).astype(bf16)
        remote(fin_s.at[k], fin.at[x], PH["fin"], {"rep_1": (x + nx - k) % nx})
    arrived("ez0", pez.at[0])
    fin[pl.ds(x, 1)] = total(pez.at[0]).astype(bf16)[None]

    arrived("info", info_r)
    arrived("lz", lgz)
    inf = info_r[...].reshape(rq, LANES)
    scale = inf[:, 0:1]
    id0, id1 = inf[:, 1:2], inf[:, 2:3]
    logits = (total(lgz) * scale)[:, 0:experts]
    lane = lax.broadcasted_iota(jnp.int32, (rq, experts), 1).astype(f32)
    zero = jnp.zeros((), f32)
    first = jnp.sum(jnp.where(lane == id0, logits, zero), axis=1, keepdims=True)
    second = jnp.sum(jnp.where(lane == id1, logits, zero), axis=1, keepdims=True)
    gate_first = sigmoid(first - second)
    gate_second = sigmoid(second - first)
    inft = inf.T
    slots = 2 * CAPACITY * nt
    slot = lax.broadcasted_iota(jnp.int32, (slots, rq), 0).astype(f32)
    token_at = lax.broadcasted_iota(jnp.int32, (slots, rq), 1)
    base = ((token_at // td) * (2 * CAPACITY)).astype(f32)
    others = fin.at[pl.ds(0, nx - 1)]
    if nx > 1:
        arrived("fin", others)
        pending.append((PH["fin"], others))
    result = jnp.zeros((slots, hid), f32)
    for e in range(2):
        gate = jnp.where(id0 == e, gate_first, zero) + jnp.where(id1 == e, gate_second, zero)
        gate = gate.astype(bf16).astype(f32)
        halves = []
        for j in range(2):
            q = 2 * e + j
            halves.append(fin[q // per_x, q % per_x].astype(f32) * scale)
        hidden = (gate * silu(halves[0]) * halves[1]).astype(bf16)
        want = inft[3 + e : 4 + e, :]
        pick = jnp.where((slot == base + want) & (want >= 0.0), 1.0, 0.0).astype(bf16)
        result = result + dot(pick, hidden)
    expert_hidden[...] = result.astype(bf16)

    for k, part in pending:
        pltpu.make_async_copy(part, part, ssem.at[k]).wait()


def shards(
    nz, nx, nt, tokens, conv_state, ssm_state, norm_gains, conv_weight, conv_skip, step_bias, decay_log,
    input_proj, select_proj, step_proj, output_proj, router, expert_proj, expert_ids,
):
    nr = nz * nx
    rows = input_proj.shape[0]
    td, model = tokens.shape
    rq = td * nt
    fb = rows * nt
    fz = fb * nx
    _, st, ch = ssm_state.shape
    hid = expert_proj.shape[3] // nt
    width = select_proj.shape[1]
    srw = -(-width // 8) * 8
    sp = -(-width * nr // LANES) * LANES
    prw = -(-(7 + st) // 8) * 8
    per_x = 4 // nx
    pieces = 3 if hid % (3 * LANES) == 0 else 2 if hid % 2 == 0 else 1
    hc = hid // pieces
    oc = output_proj.shape[1]

    V = pltpu.VMEM
    experts = router.shape[1]
    small = (
        tokens, norm_gains, conv_weight, conv_skip, step_bias[None], decay_log, step_proj, router, expert_ids,
    )
    large = (input_proj, select_proj.T, output_proj.T, expert_proj, conv_state, ssm_state)
    scratch = {"load%d" % k: (a.shape, a.dtype) for k, a in enumerate(large)}
    scratch.update(
        x1=((nr, td, fb), bf16), xb=((nz, td, fz), bf16), x2=((nt, nr, td, fb), bf16),
        xx=((nx, nz, rq, fb), bf16),
        rs_s=((td, LANES), f32), rs_r=((nt, td, LANES), f32),
        wi_s=((2, rows, nt * ch), bf16), wi_r=((2, nt, rows, ch), bf16),
        gn_s=((2, LANES), bf16), gn_r=((nt, 2, LANES), bf16), gn_b=((2, fb), bf16), gn_x=((nx, 2, fb), bf16),
        rg_s=((rows, LANES), bf16), rg_r=((nt, rows, LANES), bf16), rg_b=((experts, fb), bf16),
        rg_x=((nx, experts, fb), bf16),
        wo_r=((nt, oc, ch), bf16), wo_x=((nx, nt, oc, ch), bf16),
        st_r=((nt, 1, ch), bf16), st_b=((nt, ch), bf16),
        st_z=((nz, nt, ch), bf16), st_x=((nx, nz, nt, ch), bf16),
        pk=((prw, LANES), f32), pr_s=((prw, LANES), bf16), pr_z=((nz, prw, LANES), bf16),
        pr_x=((nx, nz, prw, LANES), bf16), pr2=((nt, prw, LANES), bf16),
        se_s=((srw, ch), bf16), se_z=((nz, srw, ch), bf16), se_x=((nx, nz, srw, ch), bf16),
        p3=((2, nx, nz, rq, ch), bf16), p3x=((2, nx, nz, rq, ch), bf16),
        p3zs=((2, nz, rq, ch), bf16), p3z=((2, nz, rq, ch), bf16),
        we_s=((4, rows, nt * hid), bf16), we_r=((pieces, 4, nt, rows, hc), bf16),
        we_x=((pieces, nx, per_x, nt, rows, hc), bf16),
        sel_s=((rq, sp), bf16), sel_r=((nt, rq, sp), bf16),
        maps=((rq, 2 * st, LANES), f32), step_b=((rq, ch), f32), act_b=((rq, ch), f32),
        ro_b=((rq, ch), f32),
        ga_s=((rq, ch), bf16), g_z=((nz, rq, ch), bf16),
        mo_s=((nz, nt, td, fz), bf16), mc_r=((nt, nz, td, fz), bf16), y_s=((nz, td, fz), bf16),
        y2=((nt, nz, td, fz), bf16), ysx=((nz, td, fz), bf16), y2b=((nt, nz, td, fz), bf16), yo=((nz, td, fz), bf16), yx=((nx, nz, rq, fz), bf16),
        info_s=((td, LANES), f32), info_r=((nt, td, LANES), f32),
        lg=((nz, rq, LANES), bf16), lgz=((nz, rq, LANES), bf16),
        pe=((nx, nz, per_x, rq, hid), bf16), pez=((nx, nz, per_x, rq, hid), bf16),
        fin_s=((nx, per_x, rq, hid), bf16), fin=((nx, per_x, rq, hid), bf16),
    )
    scratch_shapes = [V(s, d) for s, d in scratch.values()]
    scratch_shapes += [pltpu.SemaphoreType.DMA((len(PHASES),))] * 2 + [pltpu.SemaphoreType.DMA((len(large),))]
    outs = (
        ((td, model), bf16), (conv_state.shape, bf16), (ssm_state.shape, f32),
        ((2 * CAPACITY * nt, hid), bf16),
    )
    results = pl.pallas_call(
        functools.partial(kernel, nz, nx, nt),
        out_shape=tuple(V(s, d) for s, d in outs),
        in_specs=[pl.BlockSpec(memory_space=V)] * len(small) + [pl.BlockSpec(memory_space=pl.ANY)] * len(large),
        out_specs=[pl.BlockSpec(memory_space=V)] * 4,
        scratch_shapes=scratch_shapes,
        compiler_params=pltpu.CompilerParams(
            collective_id=0, has_side_effects=True, vmem_limit_bytes=61 * 1024 * 1024
        ),
        name="step",
    )(*small, *large)
    results = [pltpu.with_memory_space_constraint(a, V) for a in results]
    return pl.pallas_call(
        write_out,
        out_shape=tuple(jax.ShapeDtypeStruct(s, d) for s, d in outs),
        in_specs=[pl.BlockSpec(memory_space=V)] * 4,
        out_specs=[pl.BlockSpec(memory_space=pl.ANY)] * 4,
        scratch_shapes=[pltpu.SemaphoreType.DMA((4,))],
        name="write_out",
    )(*results)


def solution(mesh, nz=4):
    devices = mesh.devices
    nx, nt = devices.shape[0] // nz, devices.shape[1]
    split = Mesh(devices.reshape(nz, nx, nt), REP_TP)
    return jax.shard_map(
        functools.partial(shards, nz, nx, nt),
        mesh=split,
        in_specs=(
            P(REP_TP, None),
            P(None, REP, "tp"),
            P(REP, None, "tp"),
            P(None, REP_TP),
            P(None, REP_TP),
            P(None, REP_TP),
            P(REP_TP),
            P(None, REP_TP),
            P(REP_TP, None, None),
            P("tp", REP),
            P(REP_TP, None),
            P(None, REP_TP),
            P(REP_TP, None),
            P(REP_TP, None, None, None),
            P(REP_TP, None),
        ),
        out_specs=(P(REP_TP, None), P(None, REP, "tp"), P(REP, None, "tp"), P(REP, "tp")),
        check_vma=False,
    )
```

```python
import functools

import jax
import jax.numpy as jnp
from jax import lax
from jax.experimental import pallas as pl
from jax.experimental.pallas import tpu as pltpu
from jax.sharding import Mesh
from jax.sharding import PartitionSpec as P

CAPACITY = 2
REP = ("rep_0", "rep_1")
REP_TP = ("rep_0", "rep_1", "tp")
MESH = pl.DeviceIdType.MESH
EPS = 1e-05
bf16 = jnp.bfloat16
f32 = jnp.float32
LANES = 128

PHASES = (
    "x1", "xb", "rs", "wi0", "wi1", "gn", "rg", "prz", "sez", "x2",
    "st", "wo", "we0", "we1", "we2", "stz", "p3x0", "p3x1", "p3z0", "p3z1", "prx",
    "sex", "pr2", "stx", "gnx", "rgx", "wox", "wex0", "wex1", "wex2", "selp", "sel", "self", "gz", "mc",
    "y2", "yo", "info", "lz", "yx1", "yx2", "yx3", "yx4", "wol", "wo1", "wo2", "wo3", "wo4", "ez0",
    "ez1", "ez2", "ez3", "fin",
)
PH = {name: k for k, name in enumerate(PHASES)}


def sigmoid(v):
    return 1.0 / (1.0 + jnp.exp(-v))


def silu(v):
    return v / (1.0 + jnp.exp(-v))


def softplus(v):
    return jnp.maximum(v, 0.0) + jnp.log1p(jnp.exp(-jnp.abs(v)))


def dot(a, b):
    return jnp.dot(a, b, preferred_element_type=f32)


def dot_nt(a, b):
    return lax.dot_general(a, b, (((1,), (1,)), ((), ())), preferred_element_type=f32)


def write_out(*refs):
    copies = [pltpu.make_async_copy(refs[k], refs[4 + k], refs[8].at[k]) for k in range(4)]
    for copy in copies:
        copy.start()
    for copy in copies:
        copy.wait()


def kernel(
    nz, nx, nt,
    tokens, norm_gains, conv_weight, conv_skip, step_bias, decay_log, step_row, router, expert_ids,
    input_hbm, select_hbm, output_hbm, expert_hbm, conv_hbm, ssm_hbm,
    mamba_out, conv_next, ssm_next, expert_hidden,
    input_proj, select_t, output_t, expert_proj, conv_state, ssm_state,
    x1, xb, x2, xx, rs_s, rs_r, wi_s, wi_r, gn_s, gn_r, gn_b, gn_x, rg_s, rg_r, rg_b, rg_x, wo_r, wo_x,
    st_r, st_b, st_z, st_x, pk, pr_s, pr_z, pr_x, pr2, se_s, se_z, se_x, p3, p3x, p3zs, p3z,
    we_s, we_r, we_x, sel_s, sel_p, sel_h, sel_r, sel_f, maps, step_b, act_b, ro_b, ga_s, g_z,
    mo_s, mc_r, y_s, y2, yo, yx, info_s, info_r, lg, lgz, pe, pez, fin_s, fin,
    ssem, rsem, lsem,
):
    nr = nz * nx
    z, x, t = lax.axis_index("rep_0"), lax.axis_index("rep_1"), lax.axis_index("tp")
    r = z * nx + x
    rows = input_proj.shape[0]
    fb = rows * nt
    fz = fb * nx
    ch = ssm_state.shape[2]
    st = ssm_state.shape[1]
    td = tokens.shape[0]
    rq = td * nt
    rank = nr * nt
    hid = expert_proj.shape[3] // nt
    pieces, hc = we_r.shape[0], we_r.shape[4]
    cdev = conv_weight.shape[1]
    per_x = 4 // nx
    groups = {
        "tp": (nt, t, lambda p: {"tp": p}),
        "rep": (nr, r, lambda p: {"rep_0": p // nx, "rep_1": p % nx}),
        "x": (nx, x, lambda p: {"rep_1": p}),
        "z": (nz, z, lambda p: {"rep_0": p}),
    }
    core = t % 2
    partner = {"tp": t + 1 - 2 * core}
    groups["chip"] = (nt // 2, t // 2, lambda p: {"tp": p * 2 + core})
    pending = []

    def remote(src, dst, k, device):
        pltpu.make_async_remote_copy(
            src_ref=src, dst_ref=dst, send_sem=ssem.at[k], recv_sem=rsem.at[k],
            device_id=device, device_id_type=MESH,
        ).start()

    def send(group, name, src, dst, at=None, part=None):
        n, me, dev = groups[group]
        k = PH[name]
        at = at or (lambda me: dst.at[me])

        def body(step, carry):
            peer = (me + step) % n
            remote(src(peer), at(me), k, dev(peer))
            return carry

        if n > 1:
            lax.fori_loop(1, n, body, 0)
            pending.append((k, dst.at[pl.ds(0, n - 1)] if part is None else part))
        pltpu.make_async_copy(src(me), at(me), rsem.at[k]).start()

    def arrived(name, dst):
        pltpu.make_async_copy(dst, dst, rsem.at[PH[name]]).wait()

    def cols(ref, p, width):
        return ref.at[:, pl.ds(pl.multiple_of(p * width, width), width)]

    def total(ref):
        acc = ref[0].astype(f32)
        for k in range(1, ref.shape[0]):
            acc = acc + ref[k].astype(f32)
        return acc

    barrier = pltpu.get_barrier_semaphore()
    for group in ("tp", "rep"):
        n, me, dev = groups[group]

        def greet(step, carry, n=n, me=me, dev=dev):
            pl.semaphore_signal(barrier, inc=1, device_id=dev((me + step) % n), device_id_type=MESH)
            return carry

        lax.fori_loop(1, n, greet, 0)

    loads = {}
    for k, (name, src, dst) in enumerate((
        ("input", input_hbm, input_proj), ("select", select_hbm, select_t), ("output", output_hbm, output_t),
        ("expert", expert_hbm, expert_proj), ("conv", conv_hbm, conv_state), ("ssm", ssm_hbm, ssm_state),
    )):
        loads[name] = pltpu.make_async_copy(src, dst, lsem.at[k])
        loads[name].start()

    gn_s[...] = jnp.zeros(gn_s.shape, bf16)
    gn_s[:, 0:rows] = norm_gains[...]

    def send_input(j):
        wi_s[j] = input_proj[:, j, :]
        send("tp", "wi%d" % j, lambda p: cols(wi_s.at[j], p, ch), wi_r.at[j])

    def send_experts(e):
        dst = we_r.at[e]
        send(
            "tp", "we%d" % e,
            lambda p: we_s.at[:, :, pl.ds(pl.multiple_of(p * hid + e * hc, hc), hc)], dst,
            at=lambda me: dst.at[:, me], part=dst.at[:, pl.ds(0, nt - 1)],
        )

    def pass_experts(e):
        arrived("we%d" % e, we_r.at[e])
        send("x", "wex%d" % e, lambda p: we_r.at[e, pl.ds(p * per_x, per_x)], we_x.at[e])

    def lay_experts(e):
        for j in range(2):
            we_s[2 * e + j] = expert_proj[:, e, j, :]

    xf = tokens[...].astype(f32)
    rs = lax.rsqrt(jnp.mean(xf * xf, axis=1, keepdims=True) + EPS)
    rs_s[...] = jnp.broadcast_to(rs, (td, LANES))
    pl.semaphore_wait(barrier, nt - 1 + nr - 1)
    send("rep", "x1", lambda p: cols(tokens, p, fb), x1)
    send("tp", "gn", lambda p: gn_s, gn_r)
    send("tp", "rs", lambda p: rs_s, rs_r)
    send("tp", "st", lambda p: cols(step_row, p, ch), st_r)
    pk[...] = jnp.zeros(pk.shape, f32)
    pk[0:4, 0:cdev] = conv_weight[...].astype(f32)
    pk[4:6, 0:cdev] = conv_skip[...].astype(f32)
    pk[6:7, 0:cdev] = step_bias[...].astype(f32)
    pk[7 : 7 + st, 0:cdev] = decay_log[...].astype(f32)
    pr_s[...] = pk[...].astype(bf16)
    send("z", "prz", lambda p: pr_s, pr_z)
    se_s[...] = jnp.zeros(se_s.shape, bf16)
    loads["select"].wait()
    se_s[0 : select_t.shape[0], :] = select_t[...]
    send("z", "sez", lambda p: se_s, se_z)
    loads["input"].wait()
    send_input(0)
    rg_s[...] = jnp.zeros(rg_s.shape, bf16)
    rg_s[:, 0 : router.shape[1]] = router[...]
    arrived("x1", x1)
    send("tp", "x2", lambda p: x1, x2)
    send_input(1)
    loads["output"].wait()
    send("tp", "wo", lambda p: cols(output_t, p, ch), wo_r)
    send("z", "xb", lambda p: cols(tokens, p, fz), xb)
    arrived("st", st_r)
    st_b[...] = st_r[...].astype(f32).reshape(nt, ch).astype(bf16)
    send("z", "stz", lambda p: st_b, st_z)
    arrived("prz", pr_z)
    send("x", "prx", lambda p: pr_z, pr_x)
    loads["expert"].wait()
    lay_experts(0)
    arrived("sez", se_z)
    send("x", "sex", lambda p: se_z, se_x)
    lay_experts(1)
    arrived("prx", pr_x)
    send("tp", "pr2", lambda p: pr_x.at[p % nx, p // nx], pr2)
    send_experts(0)

    arrived("gn", gn_r)
    gnv = gn_r[...].astype(f32)
    gains = jnp.concatenate([gnv[k][:, 0:rows] for k in range(nt)], axis=1)
    gn_b[...] = gains.astype(bf16)
    gain0 = gains[0:1, :]
    arrived("x2", x2)

    def place_in(q, carry):
        block = x2[:, q].reshape(rq, fb).astype(f32)
        xx[q % nx, q // nx] = (block * gain0).astype(bf16)
        return carry

    lax.fori_loop(0, nr, place_in, 0)
    lhs = xx[...].reshape(nr * rq, fb)

    def partial_in(j):
        arrived("wi%d" % j, wi_r.at[j])
        p3[j] = dot(lhs, wi_r[j].reshape(fb, ch)).astype(bf16).reshape(nx, nz, rq, ch)

    def send_in(j):
        send("x", "p3x%d" % j, lambda p: p3.at[j, p], p3x.at[j])

    def sum_in(j):
        arrived("p3x%d" % j, p3x.at[j])
        p3zs[j] = total(p3x.at[j]).astype(bf16)
        send("z", "p3z%d" % j, lambda p: p3zs.at[j, p], p3z.at[j])

    partial_in(0)
    send_in(0)

    partial_in(1)
    send_in(1)
    sum_in(0)
    arrived("stz", st_z)
    send("x", "stx", lambda p: st_z, st_x)
    send("tp", "rg", lambda p: rg_s, rg_r)
    arrived("wo", wo_r)
    right, left_x = {"rep_1": (x + 1) % nx}, {"rep_1": (x + nx - 1) % nx}
    relay = nx == 4
    oh = nt // 2
    if relay:
        remote(wo_r, wo_x.at[x], PH["wo1"], right)
        remote(wo_r, wo_x.at[x], PH["wo2"], left_x)
        pltpu.make_async_copy(wo_r, wo_x.at[x], rsem.at[PH["wol"]]).start()
        pending.extend([(PH["wo1"], wo_r), (PH["wo2"], wo_r)])
    else:
        send("x", "wox", lambda p: wo_r, wo_x)
    send("x", "gnx", lambda p: gn_b, gn_x)
    arrived("sex", se_x)
    srw = se_s.shape[0]
    sp = sel_s.shape[1]
    width = select_t.shape[0]
    shape = (sp, nr * srw)
    at_col = lax.broadcasted_iota(jnp.int32, shape, 0)
    place_of = lax.broadcasted_iota(jnp.int32, shape, 1)
    blk, off = place_of // srw, place_of % srw
    true_col = ((blk % nz) * nx + blk // nz) * width + off
    perm = jnp.where((true_col == at_col) & (off < width), 1.0, 0.0).astype(bf16)
    select_all = dot(perm, se_x[...].reshape(nr * srw, ch)).astype(bf16)
    arrived("pr2", pr2)
    prv = pr2[...].astype(f32)
    par = jnp.concatenate([prv[k][:, 0:cdev] for k in range(nt)], axis=1)
    loads["conv"].wait()
    history = jnp.sum(par[0:3][:, None, :] * conv_state[...].astype(f32), axis=0) + par[4:5]
    decay_rate = -jnp.exp(par[7 : 7 + st])
    conv_next[0] = conv_state[1]
    conv_next[1] = conv_state[2]
    arrived("rs", rs_r)
    rsv = rs_r[...].reshape(rq, LANES)[:, 0:1]
    arrived("p3z0", p3z.at[0])
    conv_input = total(p3z.at[0]) * rsv
    conv_next[2] = conv_input.astype(bf16)
    activated = silu(history + par[3:4] * conv_input)
    sel_s[...] = dot_nt(activated.astype(bf16), select_all).astype(bf16)
    rh = rq // 2
    mine = pl.ds(pl.multiple_of(core * rh, rh), rh)
    remote(sel_s.at[pl.ds(pl.multiple_of((1 - core) * rh, rh), rh)], sel_p, PH["selp"], partner)
    pending.append((PH["selp"], sel_p))
    act_b[...] = activated
    arrived("selp", sel_p)
    sel_h[...] = (sel_s[mine].astype(f32) + sel_p[...].astype(f32)).astype(bf16)
    send("chip", "sel", lambda p: sel_h, sel_r)
    sum_in(1)
    if pieces > 1:
        send_experts(1)
    arrived("rg", rg_r)
    rgt = rg_r[...].reshape(fb, LANES).astype(f32).T
    rg_b[...] = rgt[0 : rg_b.shape[0]].astype(bf16)
    send("x", "rgx", lambda p: rg_b, rg_x)
    pass_experts(0)
    loads["ssm"].wait()
    arrived("stx", st_x)
    step_all = jnp.concatenate([st_x[q % nx, q // nx] for q in range(nr)], axis=0)
    arrived("sel", sel_r)
    sel_f[core] = total(sel_r)
    remote(sel_f.at[core], sel_f.at[core], PH["self"], partner)
    pending.append((PH["self"], sel_f.at[0]))
    if relay:
        from_left, from_right = wo_x.at[(x + 3) % nx], wo_x.at[(x + 1) % nx]
        arrived("wo1", from_left)
        arrived("wo2", from_right)
        for name, part, to in (
            ("wo3", from_left.at[pl.ds(0, oh)], right), ("wo4", from_right.at[pl.ds(oh, oh)], left_x),
        ):
            remote(part, part, PH[name], to)
            pending.append((PH[name], part))
    arrived("self", sel_f.at[0])
    selected = jnp.concatenate([sel_f[0], sel_f[1]], axis=0)
    step_low = selected[:, :rank].astype(bf16)
    maps[...] = jnp.broadcast_to(selected[:, rank : rank + 2 * st][:, :, None], maps.shape)
    step_b[...] = softplus(dot(step_low, step_all) + par[6:7])

    def token(i, carry):
        s = step_b[pl.ds(i, 1), :]
        a = act_b[pl.ds(i, 1), :]
        m = maps[i]
        wide = jnp.concatenate([m] * (ch // LANES), axis=1)
        nxt = jnp.exp(s * decay_rate) * ssm_state[i] + (s * a) * wide[:st]
        ssm_next[i] = nxt
        ro_b[pl.ds(i, 1), :] = jnp.sum(nxt * wide[st:], axis=0, keepdims=True)
        return carry

    lax.fori_loop(0, rq, token, 0)
    readout = ro_b[...] + par[5:6] * activated
    arrived("p3z1", p3z.at[1])
    gate_z = total(p3z.at[1]) * rsv
    ga_s[...] = (readout * silu(gate_z)).astype(bf16)

    send("z", "gz", lambda p: ga_s, g_z)
    for e in range(2, pieces):
        send_experts(e)
    if pieces > 1:
        pass_experts(1)
    if relay:
        arrived("wol", wo_x.at[x])
        arrived("wo3", wo_x.at[(x + 2) % nx, pl.ds(0, oh)])
        arrived("wo4", wo_x.at[(x + 2) % nx, pl.ds(oh, oh)])
    else:
        arrived("wox", wo_x)
    arrived("gz", g_z)
    mo = dot_nt(g_z[...].reshape(nz * rq, ch), wo_x[...].reshape(fz, ch))
    mo_s[...] = mo.astype(bf16).reshape(nz, nt, td, fz)
    send("tp", "mc", lambda p: mo_s.at[:, p], mc_r)
    for e in range(2, pieces):
        pass_experts(e)
    arrived("xb", xb)
    arrived("mc", mc_r)
    y_s[...] = (xb[...].astype(f32) + total(mc_r)).astype(bf16)
    send("tp", "y2", lambda p: y_s, y2)
    send("z", "yo", lambda p: y_s.at[p], yo)

    arrived("gnx", gn_x)
    gain1 = jnp.concatenate([gn_x[k].astype(f32)[1:2, :] for k in range(nx)], axis=1)
    arrived("rgx", rg_x)
    experts = rg_b.shape[0]
    router_all = jnp.concatenate([rg_x[k] for k in range(nx)], axis=1)

    def place_out(src, k):
        for q in range(nz):
            block = src[:, q].reshape(rq, fz).astype(f32)
            yx[k, q] = (block * gain1).astype(bf16)

    arrived("y2", y2)
    place_out(y2, 0)
    for k in (1, 3) if relay else range(1, nx):
        remote(yx.at[0], yx.at[k], PH["yx%d" % k], {"rep_1": (x + k) % nx})
        pending.append((PH["yx%d" % k], yx.at[0]))
    for e in range(pieces):
        arrived("wex%d" % e, we_x.at[e])

    def multiply(k):
        left = yx[k].reshape(nz * rq, fz)
        for c in range(per_x):
            for e in range(pieces):
                part = dot(left, we_x[e, :, c].reshape(fz, hc))
                pe[k, :, c, :, e * hc : (e + 1) * hc] = part.astype(bf16).reshape(nz, rq, hc)

    multiply(0)
    send("z", "ez0", lambda p: pe.at[0, p], pez.at[0])
    left = yx[0].reshape(nz * rq, fz)
    lg[:, :, 0:experts] = dot_nt(left, router_all).astype(bf16).reshape(nz, rq, experts)
    send("z", "lz", lambda p: lg.at[p], lgz)

    arrived("yo", yo)
    yov = [yo[k].astype(f32) for k in range(nz)]
    square = jnp.zeros((td, 1), f32)
    for k in range(nz):
        mamba_out[:, k * fz : (k + 1) * fz] = yo[k]
        square = square + jnp.sum(yov[k] * yov[k], axis=1, keepdims=True)
    rs2 = lax.rsqrt(square * (1.0 / (nr * fb)) + EPS)
    lane = lax.broadcasted_iota(jnp.int32, (td, LANES), 1)
    ids = expert_ids[...].astype(f32)
    ida, idb = ids[:, 0:1], ids[:, 1:2]
    about = jnp.where(lane == 0, rs2, jnp.where(lane == 1, ida, idb))
    for e in range(2):
        names = jnp.where((ida == e) | (idb == e), 1.0, 0.0)
        before = [jnp.zeros((1, 1), f32)]
        for k in range(1, td):
            before.append(before[-1] + names[k - 1 : k, :])
        want = jnp.where(names > 0.0, e * CAPACITY + jnp.concatenate(before, axis=0), -1.0)
        about = jnp.where(lane == 3 + e, want, about)
    info_s[...] = about
    send("tp", "info", lambda p: info_s, info_r)

    order = (1, 3, 2) if relay else tuple(range(1, nx))
    first_rows, last_rows = pl.ds(0, rq // 2), pl.ds(rq // 2, rq // 2)
    passed = {1: ("yx2", first_rows, right), 3: ("yx4", last_rows, left_x)}
    for k in order:
        if relay and k == 2:
            arrived("yx2", yx.at[2, :, first_rows])
            arrived("yx4", yx.at[2, :, last_rows])
        else:
            arrived("yx%d" % k, yx.at[k])
        if relay and k in passed:
            name, some, to = passed[k]
            remote(yx.at[k, :, some], yx.at[2, :, some], PH[name], to)
            pending.append((PH[name], yx.at[2, :, some]))
        multiply(k)
        send("z", "ez%d" % k, lambda p, k=k: pe.at[k, p], pez.at[k])
    for k in order:
        arrived("ez%d" % k, pez.at[k])
        fin_s[k] = total(pez.at[k]).astype(bf16)
        remote(fin_s.at[k], fin.at[x], PH["fin"], {"rep_1": (x + nx - k) % nx})
    arrived("ez0", pez.at[0])
    fin[pl.ds(x, 1)] = total(pez.at[0]).astype(bf16)[None]

    arrived("info", info_r)
    arrived("lz", lgz)
    inf = info_r[...].reshape(rq, LANES)
    scale = inf[:, 0:1]
    id0, id1 = inf[:, 1:2], inf[:, 2:3]
    logits = (total(lgz) * scale)[:, 0:experts]
    lane = lax.broadcasted_iota(jnp.int32, (rq, experts), 1).astype(f32)
    zero = jnp.zeros((), f32)
    first = jnp.sum(jnp.where(lane == id0, logits, zero), axis=1, keepdims=True)
    second = jnp.sum(jnp.where(lane == id1, logits, zero), axis=1, keepdims=True)
    gate_first = sigmoid(first - second)
    gate_second = sigmoid(second - first)
    inft = inf.T
    slots = 2 * CAPACITY * nt
    slot = lax.broadcasted_iota(jnp.int32, (slots, rq), 0).astype(f32)
    token_at = lax.broadcasted_iota(jnp.int32, (slots, rq), 1)
    base = ((token_at // td) * (2 * CAPACITY)).astype(f32)
    others = fin.at[pl.ds(0, nx - 1)]
    if nx > 1:
        arrived("fin", others)
        pending.append((PH["fin"], others))
    result = jnp.zeros((slots, hid), f32)
    for e in range(2):
        gate = jnp.where(id0 == e, gate_first, zero) + jnp.where(id1 == e, gate_second, zero)
        gate = gate.astype(bf16).astype(f32)
        halves = []
        for j in range(2):
            q = 2 * e + j
            halves.append(fin[q // per_x, q % per_x].astype(f32) * scale)
        hidden = (gate * silu(halves[0]) * halves[1]).astype(bf16)
        want = inft[3 + e : 4 + e, :]
        pick = jnp.where((slot == base + want) & (want >= 0.0), 1.0, 0.0).astype(bf16)
        result = result + dot(pick, hidden)
    expert_hidden[...] = result.astype(bf16)

    for k, part in pending:
        pltpu.make_async_copy(part, part, ssem.at[k]).wait()


def shards(
    nz, nx, nt, tokens, conv_state, ssm_state, norm_gains, conv_weight, conv_skip, step_bias, decay_log,
    input_proj, select_proj, step_proj, output_proj, router, expert_proj, expert_ids,
):
    nr = nz * nx
    rows = input_proj.shape[0]
    td, model = tokens.shape
    rq = td * nt
    fb = rows * nt
    fz = fb * nx
    _, st, ch = ssm_state.shape
    hid = expert_proj.shape[3] // nt
    width = select_proj.shape[1]
    srw = -(-width // 8) * 8
    sp = -(-width * nr // LANES) * LANES
    prw = -(-(7 + st) // 8) * 8
    per_x = 4 // nx
    pieces = 3 if hid % (3 * LANES) == 0 else 2 if hid % 2 == 0 else 1
    hc = hid // pieces
    oc = output_proj.shape[1]

    V = pltpu.VMEM
    experts = router.shape[1]
    small = (
        tokens, norm_gains, conv_weight, conv_skip, step_bias[None], decay_log, step_proj, router, expert_ids,
    )
    large = (input_proj, select_proj.T, output_proj.T, expert_proj, conv_state, ssm_state)
    scratch = {"load%d" % k: (a.shape, a.dtype) for k, a in enumerate(large)}
    scratch.update(
        x1=((nr, td, fb), bf16), xb=((nz, td, fz), bf16), x2=((nt, nr, td, fb), bf16),
        xx=((nx, nz, rq, fb), bf16),
        rs_s=((td, LANES), f32), rs_r=((nt, td, LANES), f32),
        wi_s=((2, rows, nt * ch), bf16), wi_r=((2, nt, rows, ch), bf16),
        gn_s=((2, LANES), bf16), gn_r=((nt, 2, LANES), bf16), gn_b=((2, fb), bf16), gn_x=((nx, 2, fb), bf16),
        rg_s=((rows, LANES), bf16), rg_r=((nt, rows, LANES), bf16), rg_b=((experts, fb), bf16),
        rg_x=((nx, experts, fb), bf16),
        wo_r=((nt, oc, ch), bf16), wo_x=((nx, nt, oc, ch), bf16),
        st_r=((nt, 1, ch), bf16), st_b=((nt, ch), bf16),
        st_z=((nz, nt, ch), bf16), st_x=((nx, nz, nt, ch), bf16),
        pk=((prw, LANES), f32), pr_s=((prw, LANES), bf16), pr_z=((nz, prw, LANES), bf16),
        pr_x=((nx, nz, prw, LANES), bf16), pr2=((nt, prw, LANES), bf16),
        se_s=((srw, ch), bf16), se_z=((nz, srw, ch), bf16), se_x=((nx, nz, srw, ch), bf16),
        p3=((2, nx, nz, rq, ch), bf16), p3x=((2, nx, nz, rq, ch), bf16),
        p3zs=((2, nz, rq, ch), bf16), p3z=((2, nz, rq, ch), bf16),
        we_s=((4, rows, nt * hid), bf16), we_r=((pieces, 4, nt, rows, hc), bf16),
        we_x=((pieces, nx, per_x, nt, rows, hc), bf16),
        sel_s=((rq, sp), bf16), sel_p=((rq // 2, sp), bf16), sel_h=((rq // 2, sp), bf16),
        sel_r=((nt // 2, rq // 2, sp), bf16), sel_f=((2, rq // 2, sp), f32),
        maps=((rq, 2 * st, LANES), f32), step_b=((rq, ch), f32), act_b=((rq, ch), f32),
        ro_b=((rq, ch), f32),
        ga_s=((rq, ch), bf16), g_z=((nz, rq, ch), bf16),
        mo_s=((nz, nt, td, fz), bf16), mc_r=((nt, nz, td, fz), bf16), y_s=((nz, td, fz), bf16),
        y2=((nt, nz, td, fz), bf16), yo=((nz, td, fz), bf16), yx=((nx, nz, rq, fz), bf16),
        info_s=((td, LANES), f32), info_r=((nt, td, LANES), f32),
        lg=((nz, rq, LANES), bf16), lgz=((nz, rq, LANES), bf16),
        pe=((nx, nz, per_x, rq, hid), bf16), pez=((nx, nz, per_x, rq, hid), bf16),
        fin_s=((nx, per_x, rq, hid), bf16), fin=((nx, per_x, rq, hid), bf16),
    )
    scratch_shapes = [V(s, d) for s, d in scratch.values()]
    scratch_shapes += [pltpu.SemaphoreType.DMA((len(PHASES),))] * 2 + [pltpu.SemaphoreType.DMA((len(large),))]
    outs = (
        ((td, model), bf16), (conv_state.shape, bf16), (ssm_state.shape, f32),
        ((2 * CAPACITY * nt, hid), bf16),
    )
    results = pl.pallas_call(
        functools.partial(kernel, nz, nx, nt),
        out_shape=tuple(V(s, d) for s, d in outs),
        in_specs=[pl.BlockSpec(memory_space=V)] * len(small) + [pl.BlockSpec(memory_space=pl.ANY)] * len(large),
        out_specs=[pl.BlockSpec(memory_space=V)] * 4,
        scratch_shapes=scratch_shapes,
        compiler_params=pltpu.CompilerParams(
            collective_id=0, has_side_effects=True, vmem_limit_bytes=61 * 1024 * 1024
        ),
        name="step",
    )(*small, *large)
    results = [pltpu.with_memory_space_constraint(a, V) for a in results]
    return pl.pallas_call(
        write_out,
        out_shape=tuple(jax.ShapeDtypeStruct(s, d) for s, d in outs),
        in_specs=[pl.BlockSpec(memory_space=V)] * 4,
        out_specs=[pl.BlockSpec(memory_space=pl.ANY)] * 4,
        scratch_shapes=[pltpu.SemaphoreType.DMA((4,))],
        name="write_out",
    )(*results)


def solution(mesh, nz=4):
    devices = mesh.devices
    nx, nt = devices.shape[0] // nz, devices.shape[1]
    split = Mesh(devices.reshape(nz, nx, nt), REP_TP)
    return jax.shard_map(
        functools.partial(shards, nz, nx, nt),
        mesh=split,
        in_specs=(
            P(REP_TP, None),
            P(None, REP, "tp"),
            P(REP, None, "tp"),
            P(None, REP_TP),
            P(None, REP_TP),
            P(None, REP_TP),
            P(REP_TP),
            P(None, REP_TP),
            P(REP_TP, None, None),
            P("tp", REP),
            P(REP_TP, None),
            P(None, REP_TP),
            P(REP_TP, None),
            P(REP_TP, None, None, None),
            P(REP_TP, None),
        ),
        out_specs=(P(REP_TP, None), P(None, REP, "tp"), P(REP, None, "tp"), P(REP, "tp")),
        check_vma=False,
    )
```

```python
import functools

import jax
import jax.numpy as jnp
from jax import lax
from jax.experimental import pallas as pl
from jax.experimental.pallas import tpu as pltpu
from jax.sharding import Mesh
from jax.sharding import PartitionSpec as P

CAPACITY = 2
REP = ("rep_0", "rep_1")
REP_TP = ("rep_0", "rep_1", "tp")
MESH = pl.DeviceIdType.MESH
EPS = 1e-05
bf16 = jnp.bfloat16
f32 = jnp.float32
LANES = 128

PHASES = (
    "x1", "xb", "rs", "wi0", "wi1", "gn", "rg", "prz", "sez", "x2",
    "st", "wo", "we0", "we1", "we2", "stz", "p3x0", "p3x1", "p3z0", "p3z1", "prx",
    "sex", "pr2", "stx", "gnx", "rgx", "wox", "wex0", "wex1", "wex2", "selp", "sel", "self", "gz", "mc",
    "y2", "yo", "info", "lz", "yx1a", "yx1b", "yx3a", "yx3b", "yx2a", "yx2b",
    "wol", "wo1", "wo2", "wo3", "wo4", "ez0",
    "ez1a", "ez1b", "ez2a", "ez2b", "ez3a", "ez3b", "fin",
)
PH = {name: k for k, name in enumerate(PHASES)}


def sigmoid(v):
    return 1.0 / (1.0 + jnp.exp(-v))


def silu(v):
    return v / (1.0 + jnp.exp(-v))


def softplus(v):
    return jnp.maximum(v, 0.0) + jnp.log1p(jnp.exp(-jnp.abs(v)))


def dot(a, b):
    return jnp.dot(a, b, preferred_element_type=f32)


def dot_nt(a, b):
    return lax.dot_general(a, b, (((1,), (1,)), ((), ())), preferred_element_type=f32)


def write_out(*refs):
    copies = [pltpu.make_async_copy(refs[k], refs[4 + k], refs[8].at[k]) for k in range(4)]
    for copy in copies:
        copy.start()
    for copy in copies:
        copy.wait()


def kernel(
    nz, nx, nt,
    tokens, norm_gains, conv_weight, conv_skip, step_bias, decay_log, step_row, router, expert_ids,
    input_hbm, select_hbm, output_hbm, expert_hbm, conv_hbm, ssm_hbm,
    mamba_out, conv_next, ssm_next, expert_hidden,
    input_proj, select_t, output_t, expert_proj, conv_state, ssm_state,
    x1, xb, x2, xx, rs_s, rs_r, wi_s, wi_r, gn_s, gn_r, gn_b, gn_x, rg_s, rg_r, rg_b, rg_x, wo_r, wo_x,
    st_r, st_b, st_z, st_x, pk, pr_s, pr_z, pr_x, pr2, se_s, se_z, se_x, p3, p3x, p3zs, p3z,
    we_s, we_r, we_x, sel_s, sel_p, sel_h, sel_r, sel_f, maps, step_b, act_b, ro_b, ga_s, g_z,
    mo_s, mc_r, y_s, y2, yo, yx, info_s, info_r, lg, lgz, pe, pez, fin_s, fin,
    ssem, rsem, lsem,
):
    nr = nz * nx
    z, x, t = lax.axis_index("rep_0"), lax.axis_index("rep_1"), lax.axis_index("tp")
    r = z * nx + x
    rows = input_proj.shape[0]
    fb = rows * nt
    fz = fb * nx
    ch = ssm_state.shape[2]
    st = ssm_state.shape[1]
    td = tokens.shape[0]
    rq = td * nt
    rank = nr * nt
    hid = expert_proj.shape[3] // nt
    pieces, hc = we_r.shape[0], we_r.shape[4]
    cdev = conv_weight.shape[1]
    per_x = 4 // nx
    groups = {
        "tp": (nt, t, lambda p: {"tp": p}),
        "rep": (nr, r, lambda p: {"rep_0": p // nx, "rep_1": p % nx}),
        "x": (nx, x, lambda p: {"rep_1": p}),
        "z": (nz, z, lambda p: {"rep_0": p}),
    }
    core = t % 2
    partner = {"tp": t + 1 - 2 * core}
    groups["chip"] = (nt // 2, t // 2, lambda p: {"tp": p * 2 + core})
    pending = []

    def remote(src, dst, k, device):
        pltpu.make_async_remote_copy(
            src_ref=src, dst_ref=dst, send_sem=ssem.at[k], recv_sem=rsem.at[k],
            device_id=device, device_id_type=MESH,
        ).start()

    def send(group, name, src, dst, at=None, part=None):
        n, me, dev = groups[group]
        k = PH[name]
        at = at or (lambda me: dst.at[me])

        def body(step, carry):
            peer = (me + step) % n
            remote(src(peer), at(me), k, dev(peer))
            return carry

        if n > 1:
            lax.fori_loop(1, n, body, 0)
            pending.append((k, dst.at[pl.ds(0, n - 1)] if part is None else part))
        pltpu.make_async_copy(src(me), at(me), rsem.at[k]).start()

    def arrived(name, dst):
        pltpu.make_async_copy(dst, dst, rsem.at[PH[name]]).wait()

    def cols(ref, p, width):
        return ref.at[:, pl.ds(pl.multiple_of(p * width, width), width)]

    def total(ref):
        acc = ref[0].astype(f32)
        for k in range(1, ref.shape[0]):
            acc = acc + ref[k].astype(f32)
        return acc

    barrier = pltpu.get_barrier_semaphore()
    for group in ("tp", "rep"):
        n, me, dev = groups[group]

        def greet(step, carry, n=n, me=me, dev=dev):
            pl.semaphore_signal(barrier, inc=1, device_id=dev((me + step) % n), device_id_type=MESH)
            return carry

        lax.fori_loop(1, n, greet, 0)

    loads = {}
    for k, (name, src, dst) in enumerate((
        ("input", input_hbm, input_proj), ("select", select_hbm, select_t), ("output", output_hbm, output_t),
        ("expert", expert_hbm, expert_proj), ("conv", conv_hbm, conv_state), ("ssm", ssm_hbm, ssm_state),
    )):
        loads[name] = pltpu.make_async_copy(src, dst, lsem.at[k])
        loads[name].start()

    gn_s[...] = jnp.zeros(gn_s.shape, bf16)
    gn_s[:, 0:rows] = norm_gains[...]

    def send_input(j):
        wi_s[j] = input_proj[:, j, :]
        send("tp", "wi%d" % j, lambda p: cols(wi_s.at[j], p, ch), wi_r.at[j])

    def send_experts(e):
        dst = we_r.at[e]
        send(
            "tp", "we%d" % e,
            lambda p: we_s.at[:, :, pl.ds(pl.multiple_of(p * hid + e * hc, hc), hc)], dst,
            at=lambda me: dst.at[:, me], part=dst.at[:, pl.ds(0, nt - 1)],
        )

    def pass_experts(e):
        arrived("we%d" % e, we_r.at[e])
        send("x", "wex%d" % e, lambda p: we_r.at[e, pl.ds(p * per_x, per_x)], we_x.at[e])

    def lay_experts(e):
        for j in range(2):
            we_s[2 * e + j] = expert_proj[:, e, j, :]

    xf = tokens[...].astype(f32)
    rs = lax.rsqrt(jnp.mean(xf * xf, axis=1, keepdims=True) + EPS)
    rs_s[...] = jnp.broadcast_to(rs, (td, LANES))
    pl.semaphore_wait(barrier, nt - 1 + nr - 1)
    send("rep", "x1", lambda p: cols(tokens, p, fb), x1)
    send("tp", "gn", lambda p: gn_s, gn_r)
    send("tp", "rs", lambda p: rs_s, rs_r)
    send("tp", "st", lambda p: cols(step_row, p, ch), st_r)
    pk[...] = jnp.zeros(pk.shape, f32)
    pk[0:4, 0:cdev] = conv_weight[...].astype(f32)
    pk[4:6, 0:cdev] = conv_skip[...].astype(f32)
    pk[6:7, 0:cdev] = step_bias[...].astype(f32)
    pk[7 : 7 + st, 0:cdev] = decay_log[...].astype(f32)
    pr_s[...] = pk[...].astype(bf16)
    send("z", "prz", lambda p: pr_s, pr_z)
    se_s[...] = jnp.zeros(se_s.shape, bf16)
    loads["select"].wait()
    se_s[0 : select_t.shape[0], :] = select_t[...]
    send("z", "sez", lambda p: se_s, se_z)
    loads["input"].wait()
    send_input(0)
    rg_s[...] = jnp.zeros(rg_s.shape, bf16)
    rg_s[:, 0 : router.shape[1]] = router[...]
    arrived("x1", x1)
    send("tp", "x2", lambda p: x1, x2)
    send_input(1)
    loads["output"].wait()
    send("tp", "wo", lambda p: cols(output_t, p, ch), wo_r)
    send("z", "xb", lambda p: cols(tokens, p, fz), xb)
    arrived("st", st_r)
    st_b[...] = st_r[...].astype(f32).reshape(nt, ch).astype(bf16)
    send("z", "stz", lambda p: st_b, st_z)
    arrived("prz", pr_z)
    send("x", "prx", lambda p: pr_z, pr_x)
    loads["expert"].wait()
    lay_experts(0)
    arrived("sez", se_z)
    send("x", "sex", lambda p: se_z, se_x)
    lay_experts(1)
    arrived("prx", pr_x)
    send("tp", "pr2", lambda p: pr_x.at[p % nx, p // nx], pr2)
    send_experts(0)

    arrived("gn", gn_r)
    gnv = gn_r[...].astype(f32)
    gains = jnp.concatenate([gnv[k][:, 0:rows] for k in range(nt)], axis=1)
    gn_b[...] = gains.astype(bf16)
    gain0 = gains[0:1, :]
    arrived("x2", x2)

    def place_in(q, carry):
        block = x2[:, q].reshape(rq, fb).astype(f32)
        xx[q % nx, q // nx] = (block * gain0).astype(bf16)
        return carry

    lax.fori_loop(0, nr, place_in, 0)
    lhs = xx[...].reshape(nr * rq, fb)

    def partial_in(j):
        arrived("wi%d" % j, wi_r.at[j])
        p3[j] = dot(lhs, wi_r[j].reshape(fb, ch)).astype(bf16).reshape(nx, nz, rq, ch)

    def send_in(j):
        send("x", "p3x%d" % j, lambda p: p3.at[j, p], p3x.at[j])

    def sum_in(j):
        arrived("p3x%d" % j, p3x.at[j])
        p3zs[j] = total(p3x.at[j]).astype(bf16)
        send("z", "p3z%d" % j, lambda p: p3zs.at[j, p], p3z.at[j])

    partial_in(0)
    send_in(0)

    partial_in(1)
    send_in(1)
    sum_in(0)
    arrived("stz", st_z)
    send("x", "stx", lambda p: st_z, st_x)
    send("tp", "rg", lambda p: rg_s, rg_r)
    arrived("wo", wo_r)
    right, left_x = {"rep_1": (x + 1) % nx}, {"rep_1": (x + nx - 1) % nx}
    relay = nx == 4
    oh = nt // 2
    if relay:
        remote(wo_r, wo_x.at[x], PH["wo1"], right)
        remote(wo_r, wo_x.at[x], PH["wo2"], left_x)
        pltpu.make_async_copy(wo_r, wo_x.at[x], rsem.at[PH["wol"]]).start()
        pending.extend([(PH["wo1"], wo_r), (PH["wo2"], wo_r)])
    else:
        send("x", "wox", lambda p: wo_r, wo_x)
    send("x", "gnx", lambda p: gn_b, gn_x)
    arrived("sex", se_x)
    srw = se_s.shape[0]
    sp = sel_s.shape[1]
    width = select_t.shape[0]
    shape = (sp, nr * srw)
    at_col = lax.broadcasted_iota(jnp.int32, shape, 0)
    place_of = lax.broadcasted_iota(jnp.int32, shape, 1)
    blk, off = place_of // srw, place_of % srw
    true_col = ((blk % nz) * nx + blk // nz) * width + off
    perm = jnp.where((true_col == at_col) & (off < width), 1.0, 0.0).astype(bf16)
    select_all = dot(perm, se_x[...].reshape(nr * srw, ch)).astype(bf16)
    arrived("pr2", pr2)
    prv = pr2[...].astype(f32)
    par = jnp.concatenate([prv[k][:, 0:cdev] for k in range(nt)], axis=1)
    loads["conv"].wait()
    history = jnp.sum(par[0:3][:, None, :] * conv_state[...].astype(f32), axis=0) + par[4:5]
    decay_rate = -jnp.exp(par[7 : 7 + st])
    conv_next[0] = conv_state[1]
    conv_next[1] = conv_state[2]
    arrived("rs", rs_r)
    rsv = rs_r[...].reshape(rq, LANES)[:, 0:1]
    arrived("p3z0", p3z.at[0])
    conv_input = total(p3z.at[0]) * rsv
    conv_next[2] = conv_input.astype(bf16)
    activated = silu(history + par[3:4] * conv_input)
    sel_s[...] = dot_nt(activated.astype(bf16), select_all).astype(bf16)
    rh = rq // 2
    mine = pl.ds(pl.multiple_of(core * rh, rh), rh)
    remote(sel_s.at[pl.ds(pl.multiple_of((1 - core) * rh, rh), rh)], sel_p, PH["selp"], partner)
    pending.append((PH["selp"], sel_p))
    act_b[...] = activated
    arrived("selp", sel_p)
    sel_h[...] = (sel_s[mine].astype(f32) + sel_p[...].astype(f32)).astype(bf16)
    send("chip", "sel", lambda p: sel_h, sel_r)
    sum_in(1)
    if pieces > 1:
        send_experts(1)
    arrived("rg", rg_r)
    rgt = rg_r[...].reshape(fb, LANES).astype(f32).T
    rg_b[...] = rgt[0 : rg_b.shape[0]].astype(bf16)
    send("x", "rgx", lambda p: rg_b, rg_x)
    pass_experts(0)
    loads["ssm"].wait()
    arrived("stx", st_x)
    step_all = jnp.concatenate([st_x[q % nx, q // nx] for q in range(nr)], axis=0)
    arrived("sel", sel_r)
    sel_f[core] = total(sel_r)
    remote(sel_f.at[core], sel_f.at[core], PH["self"], partner)
    pending.append((PH["self"], sel_f.at[0]))
    if relay:
        from_left, from_right = wo_x.at[(x + 3) % nx], wo_x.at[(x + 1) % nx]
        arrived("wo1", from_left)
        arrived("wo2", from_right)
        for name, part, to in (
            ("wo3", from_left.at[pl.ds(0, oh)], right), ("wo4", from_right.at[pl.ds(oh, oh)], left_x),
        ):
            remote(part, part, PH[name], to)
            pending.append((PH[name], part))
    arrived("self", sel_f.at[0])
    selected = jnp.concatenate([sel_f[0], sel_f[1]], axis=0)
    step_low = selected[:, :rank].astype(bf16)
    maps[...] = jnp.broadcast_to(selected[:, rank : rank + 2 * st][:, :, None], maps.shape)
    step_b[...] = softplus(dot(step_low, step_all) + par[6:7])

    def token(i, carry):
        s = step_b[pl.ds(i, 1), :]
        a = act_b[pl.ds(i, 1), :]
        m = maps[i]
        wide = jnp.concatenate([m] * (ch // LANES), axis=1)
        nxt = jnp.exp(s * decay_rate) * ssm_state[i] + (s * a) * wide[:st]
        ssm_next[i] = nxt
        ro_b[pl.ds(i, 1), :] = jnp.sum(nxt * wide[st:], axis=0, keepdims=True)
        return carry

    lax.fori_loop(0, rq, token, 0)
    readout = ro_b[...] + par[5:6] * activated
    arrived("p3z1", p3z.at[1])
    gate_z = total(p3z.at[1]) * rsv
    ga_s[...] = (readout * silu(gate_z)).astype(bf16)

    send("z", "gz", lambda p: ga_s, g_z)
    for e in range(2, pieces):
        send_experts(e)
    if pieces > 1:
        pass_experts(1)
    if relay:
        arrived("wol", wo_x.at[x])
        arrived("wo3", wo_x.at[(x + 2) % nx, pl.ds(0, oh)])
        arrived("wo4", wo_x.at[(x + 2) % nx, pl.ds(oh, oh)])
    else:
        arrived("wox", wo_x)
    arrived("gz", g_z)
    mo = dot_nt(g_z[...].reshape(nz * rq, ch), wo_x[...].reshape(fz, ch))
    mo_s[...] = mo.astype(bf16).reshape(nz, nt, td, fz)
    send("tp", "mc", lambda p: mo_s.at[:, p], mc_r)
    for e in range(2, pieces):
        pass_experts(e)
    arrived("xb", xb)
    arrived("mc", mc_r)
    y_s[...] = (xb[...].astype(f32) + total(mc_r)).astype(bf16)
    send("tp", "y2", lambda p: y_s, y2)
    send("z", "yo", lambda p: y_s.at[p], yo)

    arrived("gnx", gn_x)
    gain1 = jnp.concatenate([gn_x[k].astype(f32)[1:2, :] for k in range(nx)], axis=1)
    arrived("rgx", rg_x)
    experts = rg_b.shape[0]
    router_all = jnp.concatenate([rg_x[k] for k in range(nx)], axis=1)

    def place_out(src, k):
        for q in range(nz):
            block = src[:, q].reshape(rq, fz).astype(f32)
            yx[k, q] = (block * gain1).astype(bf16)

    arrived("y2", y2)
    place_out(y2, 0)
    near = (1, 3) if relay else tuple(range(1, nx))
    rh = rq // 2
    halves = {"a": pl.ds(0, rh), "b": pl.ds(rh, rh)}
    for half, some in halves.items():
        for k in near:
            name = "yx%d%s" % (k, half)
            remote(yx.at[0, :, some], yx.at[k, :, some], PH[name], {"rep_1": (x + k) % nx})
            pending.append((PH[name], yx.at[0, :, some]))
    for e in range(pieces):
        arrived("wex%d" % e, we_x.at[e])

    def multiply(k, some):
        left = yx[k, :, some].reshape(nz * some.size, fz)
        for c in range(per_x):
            for e in range(pieces):
                part = dot(left, we_x[e, :, c].reshape(fz, hc))
                pe[k, :, c, some, e * hc : (e + 1) * hc] = part.astype(bf16).reshape(nz, some.size, hc)

    multiply(0, pl.ds(0, rq))
    send("z", "ez0", lambda p: pe.at[0, p], pez.at[0])
    left = yx[0].reshape(nz * rq, fz)
    lg[:, :, 0:experts] = dot_nt(left, router_all).astype(bf16).reshape(nz, rq, experts)
    send("z", "lz", lambda p: lg.at[p], lgz)

    arrived("yo", yo)
    yov = [yo[k].astype(f32) for k in range(nz)]
    square = jnp.zeros((td, 1), f32)
    for k in range(nz):
        mamba_out[:, k * fz : (k + 1) * fz] = yo[k]
        square = square + jnp.sum(yov[k] * yov[k], axis=1, keepdims=True)
    rs2 = lax.rsqrt(square * (1.0 / (nr * fb)) + EPS)
    lane = lax.broadcasted_iota(jnp.int32, (td, LANES), 1)
    ids = expert_ids[...].astype(f32)
    ida, idb = ids[:, 0:1], ids[:, 1:2]
    about = jnp.where(lane == 0, rs2, jnp.where(lane == 1, ida, idb))
    for e in range(2):
        names = jnp.where((ida == e) | (idb == e), 1.0, 0.0)
        before = [jnp.zeros((1, 1), f32)]
        for k in range(1, td):
            before.append(before[-1] + names[k - 1 : k, :])
        want = jnp.where(names > 0.0, e * CAPACITY + jnp.concatenate(before, axis=0), -1.0)
        about = jnp.where(lane == 3 + e, want, about)
    info_s[...] = about
    send("tp", "info", lambda p: info_s, info_r)

    order = (1, 3, 2) if relay else near

    def block(k, half):
        some = halves[half]
        arrived("yx%d%s" % (k, half), yx.at[k, :, some])
        if relay and (k, half) in ((1, "a"), (3, "b")):
            remote(yx.at[k, :, some], yx.at[2, :, some], PH["yx2" + half], right if k == 1 else left_x)
            pending.append((PH["yx2" + half], yx.at[2, :, some]))
        multiply(k, some)
        send("z", "ez%d%s" % (k, half), lambda p: pe.at[k, p, :, some], pez.at[k, :, :, some])

    for half in halves:
        for k in near:
            block(k, half)
    if relay:
        for half in halves:
            block(2, half)
    for k in order:
        for half, some in halves.items():
            arrived("ez%d%s" % (k, half), pez.at[k, :, :, some])
        fin_s[k] = total(pez.at[k]).astype(bf16)
        remote(fin_s.at[k], fin.at[x], PH["fin"], {"rep_1": (x + nx - k) % nx})
    arrived("ez0", pez.at[0])
    fin[pl.ds(x, 1)] = total(pez.at[0]).astype(bf16)[None]

    arrived("info", info_r)
    arrived("lz", lgz)
    inf = info_r[...].reshape(rq, LANES)
    scale = inf[:, 0:1]
    id0, id1 = inf[:, 1:2], inf[:, 2:3]
    logits = (total(lgz) * scale)[:, 0:experts]
    lane = lax.broadcasted_iota(jnp.int32, (rq, experts), 1).astype(f32)
    zero = jnp.zeros((), f32)
    first = jnp.sum(jnp.where(lane == id0, logits, zero), axis=1, keepdims=True)
    second = jnp.sum(jnp.where(lane == id1, logits, zero), axis=1, keepdims=True)
    gate_first = sigmoid(first - second)
    gate_second = sigmoid(second - first)
    inft = inf.T
    slots = 2 * CAPACITY * nt
    slot = lax.broadcasted_iota(jnp.int32, (slots, rq), 0).astype(f32)
    token_at = lax.broadcasted_iota(jnp.int32, (slots, rq), 1)
    base = ((token_at // td) * (2 * CAPACITY)).astype(f32)
    others = fin.at[pl.ds(0, nx - 1)]
    if nx > 1:
        arrived("fin", others)
        pending.append((PH["fin"], others))
    result = jnp.zeros((slots, hid), f32)
    for e in range(2):
        gate = jnp.where(id0 == e, gate_first, zero) + jnp.where(id1 == e, gate_second, zero)
        gate = gate.astype(bf16).astype(f32)
        halves = []
        for j in range(2):
            q = 2 * e + j
            halves.append(fin[q // per_x, q % per_x].astype(f32) * scale)
        hidden = (gate * silu(halves[0]) * halves[1]).astype(bf16)
        want = inft[3 + e : 4 + e, :]
        pick = jnp.where((slot == base + want) & (want >= 0.0), 1.0, 0.0).astype(bf16)
        result = result + dot(pick, hidden)
    expert_hidden[...] = result.astype(bf16)

    for k, part in pending:
        pltpu.make_async_copy(part, part, ssem.at[k]).wait()


def shards(
    nz, nx, nt, tokens, conv_state, ssm_state, norm_gains, conv_weight, conv_skip, step_bias, decay_log,
    input_proj, select_proj, step_proj, output_proj, router, expert_proj, expert_ids,
):
    nr = nz * nx
    rows = input_proj.shape[0]
    td, model = tokens.shape
    rq = td * nt
    fb = rows * nt
    fz = fb * nx
    _, st, ch = ssm_state.shape
    hid = expert_proj.shape[3] // nt
    width = select_proj.shape[1]
    srw = -(-width // 8) * 8
    sp = -(-width * nr // LANES) * LANES
    prw = -(-(7 + st) // 8) * 8
    per_x = 4 // nx
    pieces = 3 if hid % (3 * LANES) == 0 else 2 if hid % 2 == 0 else 1
    hc = hid // pieces
    oc = output_proj.shape[1]

    V = pltpu.VMEM
    experts = router.shape[1]
    small = (
        tokens, norm_gains, conv_weight, conv_skip, step_bias[None], decay_log, step_proj, router, expert_ids,
    )
    large = (input_proj, select_proj.T, output_proj.T, expert_proj, conv_state, ssm_state)
    scratch = {"load%d" % k: (a.shape, a.dtype) for k, a in enumerate(large)}
    scratch.update(
        x1=((nr, td, fb), bf16), xb=((nz, td, fz), bf16), x2=((nt, nr, td, fb), bf16),
        xx=((nx, nz, rq, fb), bf16),
        rs_s=((td, LANES), f32), rs_r=((nt, td, LANES), f32),
        wi_s=((2, rows, nt * ch), bf16), wi_r=((2, nt, rows, ch), bf16),
        gn_s=((2, LANES), bf16), gn_r=((nt, 2, LANES), bf16), gn_b=((2, fb), bf16), gn_x=((nx, 2, fb), bf16),
        rg_s=((rows, LANES), bf16), rg_r=((nt, rows, LANES), bf16), rg_b=((experts, fb), bf16),
        rg_x=((nx, experts, fb), bf16),
        wo_r=((nt, oc, ch), bf16), wo_x=((nx, nt, oc, ch), bf16),
        st_r=((nt, 1, ch), bf16), st_b=((nt, ch), bf16),
        st_z=((nz, nt, ch), bf16), st_x=((nx, nz, nt, ch), bf16),
        pk=((prw, LANES), f32), pr_s=((prw, LANES), bf16), pr_z=((nz, prw, LANES), bf16),
        pr_x=((nx, nz, prw, LANES), bf16), pr2=((nt, prw, LANES), bf16),
        se_s=((srw, ch), bf16), se_z=((nz, srw, ch), bf16), se_x=((nx, nz, srw, ch), bf16),
        p3=((2, nx, nz, rq, ch), bf16), p3x=((2, nx, nz, rq, ch), bf16),
        p3zs=((2, nz, rq, ch), bf16), p3z=((2, nz, rq, ch), bf16),
        we_s=((4, rows, nt * hid), bf16), we_r=((pieces, 4, nt, rows, hc), bf16),
        we_x=((pieces, nx, per_x, nt, rows, hc), bf16),
        sel_s=((rq, sp), bf16), sel_p=((rq // 2, sp), bf16), sel_h=((rq // 2, sp), bf16),
        sel_r=((nt // 2, rq // 2, sp), bf16), sel_f=((2, rq // 2, sp), f32),
        maps=((rq, 2 * st, LANES), f32), step_b=((rq, ch), f32), act_b=((rq, ch), f32),
        ro_b=((rq, ch), f32),
        ga_s=((rq, ch), bf16), g_z=((nz, rq, ch), bf16),
        mo_s=((nz, nt, td, fz), bf16), mc_r=((nt, nz, td, fz), bf16), y_s=((nz, td, fz), bf16),
        y2=((nt, nz, td, fz), bf16), yo=((nz, td, fz), bf16), yx=((nx, nz, rq, fz), bf16),
        info_s=((td, LANES), f32), info_r=((nt, td, LANES), f32),
        lg=((nz, rq, LANES), bf16), lgz=((nz, rq, LANES), bf16),
        pe=((nx, nz, per_x, rq, hid), bf16), pez=((nx, nz, per_x, rq, hid), bf16),
        fin_s=((nx, per_x, rq, hid), bf16), fin=((nx, per_x, rq, hid), bf16),
    )
    scratch_shapes = [V(s, d) for s, d in scratch.values()]
    scratch_shapes += [pltpu.SemaphoreType.DMA((len(PHASES),))] * 2 + [pltpu.SemaphoreType.DMA((len(large),))]
    outs = (
        ((td, model), bf16), (conv_state.shape, bf16), (ssm_state.shape, f32),
        ((2 * CAPACITY * nt, hid), bf16),
    )
    results = pl.pallas_call(
        functools.partial(kernel, nz, nx, nt),
        out_shape=tuple(V(s, d) for s, d in outs),
        in_specs=[pl.BlockSpec(memory_space=V)] * len(small) + [pl.BlockSpec(memory_space=pl.ANY)] * len(large),
        out_specs=[pl.BlockSpec(memory_space=V)] * 4,
        scratch_shapes=scratch_shapes,
        compiler_params=pltpu.CompilerParams(
            collective_id=0, has_side_effects=True, vmem_limit_bytes=61 * 1024 * 1024
        ),
        name="step",
    )(*small, *large)
    results = [pltpu.with_memory_space_constraint(a, V) for a in results]
    return pl.pallas_call(
        write_out,
        out_shape=tuple(jax.ShapeDtypeStruct(s, d) for s, d in outs),
        in_specs=[pl.BlockSpec(memory_space=V)] * 4,
        out_specs=[pl.BlockSpec(memory_space=pl.ANY)] * 4,
        scratch_shapes=[pltpu.SemaphoreType.DMA((4,))],
        name="write_out",
    )(*results)


def solution(mesh, nz=4):
    devices = mesh.devices
    nx, nt = devices.shape[0] // nz, devices.shape[1]
    split = Mesh(devices.reshape(nz, nx, nt), REP_TP)
    return jax.shard_map(
        functools.partial(shards, nz, nx, nt),
        mesh=split,
        in_specs=(
            P(REP_TP, None),
            P(None, REP, "tp"),
            P(REP, None, "tp"),
            P(None, REP_TP),
            P(None, REP_TP),
            P(None, REP_TP),
            P(REP_TP),
            P(None, REP_TP),
            P(REP_TP, None, None),
            P("tp", REP),
            P(REP_TP, None),
            P(None, REP_TP),
            P(REP_TP, None),
            P(REP_TP, None, None, None),
            P(REP_TP, None),
        ),
        out_specs=(P(REP_TP, None), P(None, REP, "tp"), P(REP, None, "tp"), P(REP, "tp")),
        check_vma=False,
    )
```

```python
import functools

import jax
import jax.numpy as jnp
from jax import lax
from jax.experimental import pallas as pl
from jax.experimental.pallas import tpu as pltpu
from jax.sharding import Mesh
from jax.sharding import PartitionSpec as P

CAPACITY = 2
REP = ("rep_0", "rep_1")
REP_TP = ("rep_0", "rep_1", "tp")
MESH = pl.DeviceIdType.MESH
EPS = 1e-05
bf16 = jnp.bfloat16
f32 = jnp.float32
LANES = 128

PHASES = (
    "x1", "xb", "rs", "wi0", "wi1", "gn", "rg", "prz", "sez", "x2",
    "st", "wo", "we0", "we1", "we2", "stz", "p3x0", "p3x1", "p3z0", "p3z1", "prx",
    "sex", "pr2", "stx", "gnx", "rgx", "wox", "wex0", "wex1", "wex2", "selp", "sel", "self", "gz", "mc",
    "y2", "yo", "info", "lz", "yx1a", "yx1b", "yx3a", "yx3b", "yx2a", "yx2b",
    "wol", "wo1", "wo2", "wo3", "wo4", "ez0",
    "ez1a", "ez1b", "ez2a", "ez2b", "ez3a", "ez3b", "fin",
)
PH = {name: k for k, name in enumerate(PHASES)}


def sigmoid(v):
    return 1.0 / (1.0 + jnp.exp(-v))


def silu(v):
    return v / (1.0 + jnp.exp(-v))


def softplus(v):
    return jnp.maximum(v, 0.0) + jnp.log1p(jnp.exp(-jnp.abs(v)))


def dot(a, b):
    return jnp.dot(a, b, preferred_element_type=f32)


def dot_nt(a, b):
    return lax.dot_general(a, b, (((1,), (1,)), ((), ())), preferred_element_type=f32)


def write_out(*refs):
    copies = [pltpu.make_async_copy(refs[k], refs[4 + k], refs[8].at[k]) for k in range(4)]
    for copy in copies:
        copy.start()
    for copy in copies:
        copy.wait()


def kernel(
    nz, nx, nt,
    tokens, norm_gains, conv_weight, conv_skip, step_bias, decay_log, step_row, router, expert_ids,
    input_hbm, select_hbm, output_hbm, expert_hbm, conv_hbm, ssm_hbm,
    mamba_out, conv_next, ssm_next, expert_hidden,
    input_proj, select_t, output_t, expert_proj, conv_state, ssm_state,
    x1, xb, x2, xx, rs_s, rs_r, wi_s, wi_r, gn_s, gn_r, gn_b, gn_x, rg_s, rg_r, rg_b, rg_x, wo_r, wo_x,
    st_r, st_b, st_z, st_x, pk, pr_s, pr_z, pr_x, pr2, se_s, se_z, se_x, p3, p3x, p3zs, p3z,
    we_s, we_r, we_x, sel_s, sel_p, sel_h, sel_r, sel_f, maps, step_b, act_b, ro_b, ga_s, g_z,
    mo_s, mc_r, y_s, y2, yo, yx, info_s, info_r, lg, lgz, pe, pez, fin_s, fin,
    ssem, rsem, lsem,
):
    nr = nz * nx
    z, x, t = lax.axis_index("rep_0"), lax.axis_index("rep_1"), lax.axis_index("tp")
    r = z * nx + x
    rows = input_proj.shape[0]
    fb = rows * nt
    fz = fb * nx
    ch = ssm_state.shape[2]
    st = ssm_state.shape[1]
    td = tokens.shape[0]
    rq = td * nt
    rank = nr * nt
    hid = expert_proj.shape[3] // nt
    pieces, hc = we_r.shape[0], we_r.shape[4]
    cdev = conv_weight.shape[1]
    per_x = 4 // nx
    groups = {
        "tp": (nt, t, lambda p: {"tp": p}),
        "rep": (nr, r, lambda p: {"rep_0": p // nx, "rep_1": p % nx}),
        "x": (nx, x, lambda p: {"rep_1": p}),
        "z": (nz, z, lambda p: {"rep_0": p}),
    }
    core = t % 2
    partner = {"tp": t + 1 - 2 * core}
    groups["chip"] = (nt // 2, t // 2, lambda p: {"tp": p * 2 + core})
    pending = []

    def remote(src, dst, k, device):
        pltpu.make_async_remote_copy(
            src_ref=src, dst_ref=dst, send_sem=ssem.at[k], recv_sem=rsem.at[k],
            device_id=device, device_id_type=MESH,
        ).start()

    def send(group, name, src, dst, at=None, part=None):
        n, me, dev = groups[group]
        k = PH[name]
        at = at or (lambda me: dst.at[me])

        def body(step, carry):
            peer = (me + step) % n
            remote(src(peer), at(me), k, dev(peer))
            return carry

        if n > 1:
            lax.fori_loop(1, n, body, 0)
            pending.append((k, dst.at[pl.ds(0, n - 1)] if part is None else part))
        pltpu.make_async_copy(src(me), at(me), rsem.at[k]).start()

    def arrived(name, dst):
        pltpu.make_async_copy(dst, dst, rsem.at[PH[name]]).wait()

    def cols(ref, p, width):
        return ref.at[:, pl.ds(pl.multiple_of(p * width, width), width)]

    def total(ref):
        acc = ref[0].astype(f32)
        for k in range(1, ref.shape[0]):
            acc = acc + ref[k].astype(f32)
        return acc

    barrier = pltpu.get_barrier_semaphore()
    for group in ("tp", "rep"):
        n, me, dev = groups[group]

        def greet(step, carry, n=n, me=me, dev=dev):
            pl.semaphore_signal(barrier, inc=1, device_id=dev((me + step) % n), device_id_type=MESH)
            return carry

        lax.fori_loop(1, n, greet, 0)

    loads = {}
    for k, (name, src, dst) in enumerate((
        ("input", input_hbm, input_proj), ("select", select_hbm, select_t), ("output", output_hbm, output_t),
        ("expert", expert_hbm, expert_proj), ("conv", conv_hbm, conv_state), ("ssm", ssm_hbm, ssm_state),
    )):
        loads[name] = pltpu.make_async_copy(src, dst, lsem.at[k])
        loads[name].start()

    gn_s[...] = jnp.zeros(gn_s.shape, bf16)
    gn_s[:, 0:rows] = norm_gains[...]

    def send_input(j):
        wi_s[j] = input_proj[:, j, :]
        send("tp", "wi%d" % j, lambda p: cols(wi_s.at[j], p, ch), wi_r.at[j])

    def send_experts(e):
        dst = we_r.at[e]
        send(
            "tp", "we%d" % e,
            lambda p: we_s.at[:, :, pl.ds(pl.multiple_of(p * hid + e * hc, hc), hc)], dst,
            at=lambda me: dst.at[:, me], part=dst.at[:, pl.ds(0, nt - 1)],
        )

    def pass_experts(e):
        arrived("we%d" % e, we_r.at[e])
        send("x", "wex%d" % e, lambda p: we_r.at[e, pl.ds(p * per_x, per_x)], we_x.at[e])

    def lay_experts(e):
        for j in range(2):
            we_s[2 * e + j] = expert_proj[:, e, j, :]

    xf = tokens[...].astype(f32)
    rs = lax.rsqrt(jnp.mean(xf * xf, axis=1, keepdims=True) + EPS)
    rs_s[...] = jnp.broadcast_to(rs, (td, LANES))
    pl.semaphore_wait(barrier, nt - 1 + nr - 1)
    send("rep", "x1", lambda p: cols(tokens, p, fb), x1)
    send("tp", "gn", lambda p: gn_s, gn_r)
    send("tp", "rs", lambda p: rs_s, rs_r)
    send("tp", "st", lambda p: cols(step_row, p, ch), st_r)
    pk[...] = jnp.zeros(pk.shape, f32)
    pk[0:4, 0:cdev] = conv_weight[...].astype(f32)
    pk[4:6, 0:cdev] = conv_skip[...].astype(f32)
    pk[6:7, 0:cdev] = step_bias[...].astype(f32)
    pk[7 : 7 + st, 0:cdev] = decay_log[...].astype(f32)
    pr_s[...] = pk[...].astype(bf16)
    send("z", "prz", lambda p: pr_s, pr_z)
    se_s[...] = jnp.zeros(se_s.shape, bf16)
    loads["select"].wait()
    se_s[0 : select_t.shape[0], :] = select_t[...]
    send("z", "sez", lambda p: se_s, se_z)
    loads["input"].wait()
    send_input(0)
    rg_s[...] = jnp.zeros(rg_s.shape, bf16)
    rg_s[:, 0 : router.shape[1]] = router[...]
    arrived("x1", x1)
    send("tp", "x2", lambda p: x1, x2)
    send_input(1)
    loads["output"].wait()
    send("tp", "wo", lambda p: cols(output_t, p, ch), wo_r)
    send("z", "xb", lambda p: cols(tokens, p, fz), xb)
    arrived("st", st_r)
    st_b[...] = st_r[...].astype(f32).reshape(nt, ch).astype(bf16)
    send("z", "stz", lambda p: st_b, st_z)
    arrived("prz", pr_z)
    send("x", "prx", lambda p: pr_z, pr_x)
    loads["expert"].wait()
    lay_experts(0)
    arrived("sez", se_z)
    send("x", "sex", lambda p: se_z, se_x)
    lay_experts(1)
    arrived("prx", pr_x)
    send("tp", "pr2", lambda p: pr_x.at[p % nx, p // nx], pr2)
    send_experts(0)

    arrived("gn", gn_r)
    gnv = gn_r[...].astype(f32)
    gains = jnp.concatenate([gnv[k][:, 0:rows] for k in range(nt)], axis=1)
    gn_b[...] = gains.astype(bf16)
    gain0 = gains[0:1, :]
    arrived("x2", x2)

    def place_in(q, carry):
        block = x2[:, q].reshape(rq, fb).astype(f32)
        xx[q % nx, q // nx] = (block * gain0).astype(bf16)
        return carry

    lax.fori_loop(0, nr, place_in, 0)
    lhs = xx[...].reshape(nr * rq, fb)

    def partial_in(j):
        arrived("wi%d" % j, wi_r.at[j])
        p3[j] = dot(lhs, wi_r[j].reshape(fb, ch)).astype(bf16).reshape(nx, nz, rq, ch)

    def send_in(j):
        send("x", "p3x%d" % j, lambda p: p3.at[j, p], p3x.at[j])

    def sum_in(j):
        arrived("p3x%d" % j, p3x.at[j])
        p3zs[j] = total(p3x.at[j]).astype(bf16)
        send("z", "p3z%d" % j, lambda p: p3zs.at[j, p], p3z.at[j])

    partial_in(0)
    send_in(0)

    partial_in(1)
    send_in(1)
    sum_in(0)
    arrived("stz", st_z)
    send("x", "stx", lambda p: st_z, st_x)
    send("tp", "rg", lambda p: rg_s, rg_r)
    arrived("wo", wo_r)
    right, left_x = {"rep_1": (x + 1) % nx}, {"rep_1": (x + nx - 1) % nx}
    relay = nx == 4
    oh = nt // 2
    if relay:
        remote(wo_r, wo_x.at[x], PH["wo1"], right)
        remote(wo_r, wo_x.at[x], PH["wo2"], left_x)
        pltpu.make_async_copy(wo_r, wo_x.at[x], rsem.at[PH["wol"]]).start()
        pending.extend([(PH["wo1"], wo_r), (PH["wo2"], wo_r)])
    else:
        send("x", "wox", lambda p: wo_r, wo_x)
    send("x", "gnx", lambda p: gn_b, gn_x)
    arrived("sex", se_x)
    srw = se_s.shape[0]
    sp = sel_s.shape[1]
    width = select_t.shape[0]
    shape = (sp, nr * srw)
    at_col = lax.broadcasted_iota(jnp.int32, shape, 0)
    place_of = lax.broadcasted_iota(jnp.int32, shape, 1)
    blk, off = place_of // srw, place_of % srw
    true_col = ((blk % nz) * nx + blk // nz) * width + off
    perm = jnp.where((true_col == at_col) & (off < width), 1.0, 0.0).astype(bf16)
    select_all = dot(perm, se_x[...].reshape(nr * srw, ch)).astype(bf16)
    arrived("pr2", pr2)
    prv = pr2[...].astype(f32)
    par = jnp.concatenate([prv[k][:, 0:cdev] for k in range(nt)], axis=1)
    loads["conv"].wait()
    history = jnp.sum(par[0:3][:, None, :] * conv_state[...].astype(f32), axis=0) + par[4:5]
    decay_rate = -jnp.exp(par[7 : 7 + st])
    conv_next[0] = conv_state[1]
    conv_next[1] = conv_state[2]
    arrived("rs", rs_r)
    rsv = rs_r[...].reshape(rq, LANES)[:, 0:1]
    arrived("p3z0", p3z.at[0])
    conv_input = total(p3z.at[0]) * rsv
    conv_next[2] = conv_input.astype(bf16)
    activated = silu(history + par[3:4] * conv_input)
    sel_s[...] = dot_nt(activated.astype(bf16), select_all).astype(bf16)
    rh = rq // 2
    mine = pl.ds(pl.multiple_of(core * rh, rh), rh)
    remote(sel_s.at[pl.ds(pl.multiple_of((1 - core) * rh, rh), rh)], sel_p, PH["selp"], partner)
    pending.append((PH["selp"], sel_p))
    act_b[...] = activated
    arrived("selp", sel_p)
    sel_h[...] = (sel_s[mine].astype(f32) + sel_p[...].astype(f32)).astype(bf16)
    send("chip", "sel", lambda p: sel_h, sel_r)
    sum_in(1)
    if pieces > 1:
        send_experts(1)
    arrived("rg", rg_r)
    rgt = rg_r[...].reshape(fb, LANES).astype(f32).T
    rg_b[...] = rgt[0 : rg_b.shape[0]].astype(bf16)
    send("x", "rgx", lambda p: rg_b, rg_x)
    pass_experts(0)
    loads["ssm"].wait()
    arrived("stx", st_x)
    step_all = jnp.concatenate([st_x[q % nx, q // nx] for q in range(nr)], axis=0)
    arrived("sel", sel_r)
    sel_f[core] = total(sel_r)
    remote(sel_f.at[core], sel_f.at[core], PH["self"], partner)
    pending.append((PH["self"], sel_f.at[0]))
    if relay:
        from_left, from_right = wo_x.at[(x + 3) % nx], wo_x.at[(x + 1) % nx]
        arrived("wo1", from_left)
        arrived("wo2", from_right)
        for name, part, to in (
            ("wo3", from_left.at[pl.ds(0, oh)], right), ("wo4", from_right.at[pl.ds(oh, oh)], left_x),
        ):
            remote(part, part, PH[name], to)
            pending.append((PH[name], part))
    arrived("self", sel_f.at[0])
    selected = jnp.concatenate([sel_f[0], sel_f[1]], axis=0)
    step_low = selected[:, :rank].astype(bf16)
    maps[...] = jnp.broadcast_to(selected[:, rank : rank + 2 * st][:, :, None], maps.shape)
    step_b[...] = softplus(dot(step_low, step_all) + par[6:7])

    def token(i, carry):
        s = step_b[pl.ds(i, 1), :]
        a = act_b[pl.ds(i, 1), :]
        m = maps[i]
        wide = jnp.concatenate([m] * (ch // LANES), axis=1)
        nxt = jnp.exp(s * decay_rate) * ssm_state[i] + (s * a) * wide[:st]
        ssm_next[i] = nxt
        ro_b[pl.ds(i, 1), :] = jnp.sum(nxt * wide[st:], axis=0, keepdims=True)
        return carry

    lax.fori_loop(0, rq, token, 0)
    readout = ro_b[...] + par[5:6] * activated
    arrived("p3z1", p3z.at[1])
    gate_z = total(p3z.at[1]) * rsv
    ga_s[...] = (readout * silu(gate_z)).astype(bf16)

    send("z", "gz", lambda p: ga_s, g_z)
    for e in range(2, pieces):
        send_experts(e)
    if pieces > 1:
        pass_experts(1)
    if relay:
        arrived("wol", wo_x.at[x])
        arrived("wo3", wo_x.at[(x + 2) % nx, pl.ds(0, oh)])
        arrived("wo4", wo_x.at[(x + 2) % nx, pl.ds(oh, oh)])
    else:
        arrived("wox", wo_x)
    arrived("gz", g_z)
    mo = dot_nt(g_z[...].reshape(nz * rq, ch), wo_x[...].reshape(fz, ch))
    mo_s[...] = mo.astype(bf16).reshape(nz, nt, td, fz)
    send("tp", "mc", lambda p: mo_s.at[:, p], mc_r)
    for e in range(2, pieces):
        pass_experts(e)
    arrived("xb", xb)
    arrived("mc", mc_r)
    y_s[...] = (xb[...].astype(f32) + total(mc_r)).astype(bf16)
    send("tp", "y2", lambda p: y_s, y2)
    send("z", "yo", lambda p: y_s.at[p], yo)

    arrived("gnx", gn_x)
    gain1 = jnp.concatenate([gn_x[k].astype(f32)[1:2, :] for k in range(nx)], axis=1)
    arrived("rgx", rg_x)
    experts = rg_b.shape[0]
    router_all = jnp.concatenate([rg_x[k] for k in range(nx)], axis=1)

    def place_out(src, k):
        for q in range(nz):
            block = src[:, q].reshape(rq, fz).astype(f32)
            yx[k, q] = (block * gain1).astype(bf16)

    arrived("y2", y2)
    place_out(y2, 0)
    near = (1, 3) if relay else tuple(range(1, nx))
    rh = rq // 2
    halves = {"a": pl.ds(0, rh), "b": pl.ds(rh, rh)}
    for half, some in halves.items():
        for k in near:
            name = "yx%d%s" % (k, half)
            remote(yx.at[0, :, some], yx.at[k, :, some], PH[name], {"rep_1": (x + k) % nx})
            pending.append((PH[name], yx.at[0, :, some]))
    for e in range(pieces):
        arrived("wex%d" % e, we_x.at[e])

    def multiply(k, some):
        left = yx[k, :, some].reshape(nz * some.size, fz)
        for c in range(per_x):
            for e in range(pieces):
                part = dot(left, we_x[e, :, c].reshape(fz, hc))
                pe[k, :, c, some, e * hc : (e + 1) * hc] = part.astype(bf16).reshape(nz, some.size, hc)

    multiply(0, pl.ds(0, rq))
    send("z", "ez0", lambda p: pe.at[0, p], pez.at[0])
    left = yx[0].reshape(nz * rq, fz)
    lg[:, :, 0:experts] = dot_nt(left, router_all).astype(bf16).reshape(nz, rq, experts)
    send("z", "lz", lambda p: lg.at[p], lgz)

    arrived("yo", yo)
    yov = [yo[k].astype(f32) for k in range(nz)]
    square = jnp.zeros((td, 1), f32)
    for k in range(nz):
        mamba_out[:, k * fz : (k + 1) * fz] = yo[k]
        square = square + jnp.sum(yov[k] * yov[k], axis=1, keepdims=True)
    rs2 = lax.rsqrt(square * (1.0 / (nr * fb)) + EPS)
    lane = lax.broadcasted_iota(jnp.int32, (td, LANES), 1)
    ids = expert_ids[...].astype(f32)
    ida, idb = ids[:, 0:1], ids[:, 1:2]
    about = jnp.where(lane == 0, rs2, jnp.where(lane == 1, ida, idb))
    for e in range(2):
        names = jnp.where((ida == e) | (idb == e), 1.0, 0.0)
        before = [jnp.zeros((1, 1), f32)]
        for k in range(1, td):
            before.append(before[-1] + names[k - 1 : k, :])
        want = jnp.where(names > 0.0, e * CAPACITY + jnp.concatenate(before, axis=0), -1.0)
        about = jnp.where(lane == 3 + e, want, about)
    info_s[...] = about
    send("tp", "info", lambda p: info_s, info_r)

    order = (1, 3, 2) if relay else near

    def block(k, half):
        some = halves[half]
        arrived("yx%d%s" % (k, half), yx.at[k, :, some])
        if relay and (k, half) in ((1, "a"), (3, "b")):
            remote(yx.at[k, :, some], yx.at[2, :, some], PH["yx2" + half], right if k == 1 else left_x)
            pending.append((PH["yx2" + half], yx.at[2, :, some]))
        multiply(k, some)
        send("z", "ez%d%s" % (k, half), lambda p: pe.at[k, p, :, some], pez.at[k, :, :, some])

    for half in halves:
        for k in near:
            block(k, half)
    if relay:
        for half in halves:
            block(2, half)
    for k in order:
        for half, some in halves.items():
            arrived("ez%d%s" % (k, half), pez.at[k, :, :, some])
            fin_s[k, :, some] = total(pez.at[k, :, :, some]).astype(bf16)
            remote(
                fin_s.at[k, :, some], fin.at[x, :, some], PH["fin"], {"rep_1": (x + nx - k) % nx}
            )
    arrived("ez0", pez.at[0])
    fin[pl.ds(x, 1)] = total(pez.at[0]).astype(bf16)[None]

    arrived("info", info_r)
    arrived("lz", lgz)
    inf = info_r[...].reshape(rq, LANES)
    scale = inf[:, 0:1]
    id0, id1 = inf[:, 1:2], inf[:, 2:3]
    logits = (total(lgz) * scale)[:, 0:experts]
    lane = lax.broadcasted_iota(jnp.int32, (rq, experts), 1).astype(f32)
    zero = jnp.zeros((), f32)
    first = jnp.sum(jnp.where(lane == id0, logits, zero), axis=1, keepdims=True)
    second = jnp.sum(jnp.where(lane == id1, logits, zero), axis=1, keepdims=True)
    gate_first = sigmoid(first - second)
    gate_second = sigmoid(second - first)
    inft = inf.T
    slots = 2 * CAPACITY * nt
    slot = lax.broadcasted_iota(jnp.int32, (slots, rq), 0).astype(f32)
    token_at = lax.broadcasted_iota(jnp.int32, (slots, rq), 1)
    base = ((token_at // td) * (2 * CAPACITY)).astype(f32)
    others = fin.at[pl.ds(0, nx - 1)]
    if nx > 1:
        arrived("fin", others)
        pending.append((PH["fin"], others))
    result = jnp.zeros((slots, hid), f32)
    for e in range(2):
        gate = jnp.where(id0 == e, gate_first, zero) + jnp.where(id1 == e, gate_second, zero)
        gate = gate.astype(bf16).astype(f32)
        halves = []
        for j in range(2):
            q = 2 * e + j
            halves.append(fin[q // per_x, q % per_x].astype(f32) * scale)
        hidden = (gate * silu(halves[0]) * halves[1]).astype(bf16)
        want = inft[3 + e : 4 + e, :]
        pick = jnp.where((slot == base + want) & (want >= 0.0), 1.0, 0.0).astype(bf16)
        result = result + dot(pick, hidden)
    expert_hidden[...] = result.astype(bf16)

    for k, part in pending:
        pltpu.make_async_copy(part, part, ssem.at[k]).wait()


def shards(
    nz, nx, nt, tokens, conv_state, ssm_state, norm_gains, conv_weight, conv_skip, step_bias, decay_log,
    input_proj, select_proj, step_proj, output_proj, router, expert_proj, expert_ids,
):
    nr = nz * nx
    rows = input_proj.shape[0]
    td, model = tokens.shape
    rq = td * nt
    fb = rows * nt
    fz = fb * nx
    _, st, ch = ssm_state.shape
    hid = expert_proj.shape[3] // nt
    width = select_proj.shape[1]
    srw = -(-width // 8) * 8
    sp = -(-width * nr // LANES) * LANES
    prw = -(-(7 + st) // 8) * 8
    per_x = 4 // nx
    pieces = 3 if hid % (3 * LANES) == 0 else 2 if hid % 2 == 0 else 1
    hc = hid // pieces
    oc = output_proj.shape[1]

    V = pltpu.VMEM
    experts = router.shape[1]
    small = (
        tokens, norm_gains, conv_weight, conv_skip, step_bias[None], decay_log, step_proj, router, expert_ids,
    )
    large = (input_proj, select_proj.T, output_proj.T, expert_proj, conv_state, ssm_state)
    scratch = {"load%d" % k: (a.shape, a.dtype) for k, a in enumerate(large)}
    scratch.update(
        x1=((nr, td, fb), bf16), xb=((nz, td, fz), bf16), x2=((nt, nr, td, fb), bf16),
        xx=((nx, nz, rq, fb), bf16),
        rs_s=((td, LANES), f32), rs_r=((nt, td, LANES), f32),
        wi_s=((2, rows, nt * ch), bf16), wi_r=((2, nt, rows, ch), bf16),
        gn_s=((2, LANES), bf16), gn_r=((nt, 2, LANES), bf16), gn_b=((2, fb), bf16), gn_x=((nx, 2, fb), bf16),
        rg_s=((rows, LANES), bf16), rg_r=((nt, rows, LANES), bf16), rg_b=((experts, fb), bf16),
        rg_x=((nx, experts, fb), bf16),
        wo_r=((nt, oc, ch), bf16), wo_x=((nx, nt, oc, ch), bf16),
        st_r=((nt, 1, ch), bf16), st_b=((nt, ch), bf16),
        st_z=((nz, nt, ch), bf16), st_x=((nx, nz, nt, ch), bf16),
        pk=((prw, LANES), f32), pr_s=((prw, LANES), bf16), pr_z=((nz, prw, LANES), bf16),
        pr_x=((nx, nz, prw, LANES), bf16), pr2=((nt, prw, LANES), bf16),
        se_s=((srw, ch), bf16), se_z=((nz, srw, ch), bf16), se_x=((nx, nz, srw, ch), bf16),
        p3=((2, nx, nz, rq, ch), bf16), p3x=((2, nx, nz, rq, ch), bf16),
        p3zs=((2, nz, rq, ch), bf16), p3z=((2, nz, rq, ch), bf16),
        we_s=((4, rows, nt * hid), bf16), we_r=((pieces, 4, nt, rows, hc), bf16),
        we_x=((pieces, nx, per_x, nt, rows, hc), bf16),
        sel_s=((rq, sp), bf16), sel_p=((rq // 2, sp), bf16), sel_h=((rq // 2, sp), bf16),
        sel_r=((nt // 2, rq // 2, sp), bf16), sel_f=((2, rq // 2, sp), f32),
        maps=((rq, 2 * st, LANES), f32), step_b=((rq, ch), f32), act_b=((rq, ch), f32),
        ro_b=((rq, ch), f32),
        ga_s=((rq, ch), bf16), g_z=((nz, rq, ch), bf16),
        mo_s=((nz, nt, td, fz), bf16), mc_r=((nt, nz, td, fz), bf16), y_s=((nz, td, fz), bf16),
        y2=((nt, nz, td, fz), bf16), yo=((nz, td, fz), bf16), yx=((nx, nz, rq, fz), bf16),
        info_s=((td, LANES), f32), info_r=((nt, td, LANES), f32),
        lg=((nz, rq, LANES), bf16), lgz=((nz, rq, LANES), bf16),
        pe=((nx, nz, per_x, rq, hid), bf16), pez=((nx, nz, per_x, rq, hid), bf16),
        fin_s=((nx, per_x, rq, hid), bf16), fin=((nx, per_x, rq, hid), bf16),
    )
    scratch_shapes = [V(s, d) for s, d in scratch.values()]
    scratch_shapes += [pltpu.SemaphoreType.DMA((len(PHASES),))] * 2 + [pltpu.SemaphoreType.DMA((len(large),))]
    outs = (
        ((td, model), bf16), (conv_state.shape, bf16), (ssm_state.shape, f32),
        ((2 * CAPACITY * nt, hid), bf16),
    )
    results = pl.pallas_call(
        functools.partial(kernel, nz, nx, nt),
        out_shape=tuple(V(s, d) for s, d in outs),
        in_specs=[pl.BlockSpec(memory_space=V)] * len(small) + [pl.BlockSpec(memory_space=pl.ANY)] * len(large),
        out_specs=[pl.BlockSpec(memory_space=V)] * 4,
        scratch_shapes=scratch_shapes,
        compiler_params=pltpu.CompilerParams(
            collective_id=0, has_side_effects=True, vmem_limit_bytes=61 * 1024 * 1024
        ),
        name="step",
    )(*small, *large)
    results = [pltpu.with_memory_space_constraint(a, V) for a in results]
    return pl.pallas_call(
        write_out,
        out_shape=tuple(jax.ShapeDtypeStruct(s, d) for s, d in outs),
        in_specs=[pl.BlockSpec(memory_space=V)] * 4,
        out_specs=[pl.BlockSpec(memory_space=pl.ANY)] * 4,
        scratch_shapes=[pltpu.SemaphoreType.DMA((4,))],
        name="write_out",
    )(*results)


def solution(mesh, nz=4):
    devices = mesh.devices
    nx, nt = devices.shape[0] // nz, devices.shape[1]
    split = Mesh(devices.reshape(nz, nx, nt), REP_TP)
    return jax.shard_map(
        functools.partial(shards, nz, nx, nt),
        mesh=split,
        in_specs=(
            P(REP_TP, None),
            P(None, REP, "tp"),
            P(REP, None, "tp"),
            P(None, REP_TP),
            P(None, REP_TP),
            P(None, REP_TP),
            P(REP_TP),
            P(None, REP_TP),
            P(REP_TP, None, None),
            P("tp", REP),
            P(REP_TP, None),
            P(None, REP_TP),
            P(REP_TP, None),
            P(REP_TP, None, None, None),
            P(REP_TP, None),
        ),
        out_specs=(P(REP_TP, None), P(None, REP, "tp"), P(REP, None, "tp"), P(REP, "tp")),
        check_vma=False,
    )
```
